8 devices in a mesh: dp: 2 (over z, y), ep: 4 (over x, core).
Axes of the slice: x: 2, y: 2, z: 1, core: 2. Of those that a mesh axis runs over, the one named last changes fastest.
Arguments:
- tokens: bfloat16 [2048, 2048], P(('dp', 'ep')), parts along dimension 0
- expert_ids: int32 [2048, 8], P(('dp', 'ep')), parts along dimension 0
- gate_vals: float32 [2048, 8], P(('dp', 'ep')), parts along dimension 0
- w_gate: bfloat16 [64, 2048, 1024], P('ep')
- w_up: bfloat16 [64, 2048, 1024], P('ep')
- w_down: bfloat16 [64, 1024, 2048], P('ep')
Outputs:
- output: bfloat16 [2048, 2048], P(('dp', 'ep')), parts along dimension 0
There are 2 independent parts. The reference program is written for one: setup_inputs(seed, part) draws one part's arguments, and reference() takes and returns one part's arrays. A program takes and returns all parts, laid end to end along the dimension named above; an argument that names none is the same for every part.
All inputs are finite; a program needn't handle non-finite values.
Results may differ from the reference program's by a relative error of at most 0.0063039.
Values are sent between devices in bfloat16 or wider.
A program may use at most 1 GiB of HBM per device.

```python
import jax
import jax.numpy as jnp
from jax import lax

D_MODEL = 2048
FFN_DIM = 1024
NUM_EXPERTS = 64
TOP_K = 8
GROUP = 4
TOK_DEV = 256

DEV_LIMIT = TOP_K // 2
LOCAL_EXPERTS = NUM_EXPERTS // GROUP
PAIR_CAP = TOK_DEV * DEV_LIMIT // GROUP
EXPERT_CAP = TOK_DEV * TOP_K * GROUP // NUM_EXPERTS
TOKENS = GROUP * TOK_DEV


def perm_rows(rand_key, row_count, perm_size):
    return jax.vmap(lambda sub_key: jax.random.permutation(sub_key, perm_size))(jax.random.split(rand_key, row_count))


def draw_routing(rand_key):
    key_src, key_dst, key_slot = jax.random.split(rand_key, 3)
    src_perm = perm_rows(key_src, GROUP, GROUP)
    dst_perm = perm_rows(key_dst, GROUP, LOCAL_EXPERTS)
    flat_pos = jnp.arange(TOK_DEV)[:, None] * DEV_LIMIT + jnp.arange(DEV_LIMIT)[None, :]
    dest_dev = src_perm[:, flat_pos % GROUP]
    recv_row = jnp.arange(GROUP)[:, None, None] * PAIR_CAP + (flat_pos // GROUP)[None, :, :]
    first_loc = dst_perm[dest_dev, (2 * recv_row) % LOCAL_EXPERTS]
    second_loc = dst_perm[dest_dev, (2 * recv_row + 1) % LOCAL_EXPERTS]
    pair_ids = jnp.stack([first_loc, second_loc], axis=-1) + dest_dev[..., None] * LOCAL_EXPERTS
    ordered = pair_ids.reshape(TOKENS, TOP_K)
    scores = jax.random.randint(key_slot, (TOKENS, TOP_K), 0, 1 << 20) * TOP_K + jnp.arange(TOP_K)[None, :]
    slot_order = jnp.argsort(scores, axis=1)
    return jnp.take_along_axis(ordered, slot_order, axis=1).astype(jnp.int32)


def setup_inputs(seed: int = 0, part: int = 0) -> dict:
    base_key = jax.random.key(seed)
    key_x, key_route, key_gate = jax.random.split(jax.random.fold_in(base_key, part), 3)
    key_wg, key_wu, key_wd = jax.random.split(jax.random.key(seed + 1), 3)
    in_scale = D_MODEL ** -0.5
    out_scale = 2.0 * FFN_DIM ** -0.5
    tokens = jax.random.normal(key_x, (TOKENS, D_MODEL), jnp.float32).astype(jnp.bfloat16)
    expert_ids = draw_routing(key_route)
    logits = 1.5 * jax.random.normal(key_gate, (TOKENS, TOP_K), jnp.float32)
    gate_vals = jax.nn.softmax(logits, axis=-1)
    w_gate = (in_scale * jax.random.normal(key_wg, (NUM_EXPERTS, D_MODEL, FFN_DIM), jnp.float32)).astype(jnp.bfloat16)
    w_up = (in_scale * jax.random.normal(key_wu, (NUM_EXPERTS, D_MODEL, FFN_DIM), jnp.float32)).astype(jnp.bfloat16)
    w_down = (out_scale * jax.random.normal(key_wd, (NUM_EXPERTS, FFN_DIM, D_MODEL), jnp.float32)).astype(jnp.bfloat16)
    return {'tokens': tokens, 'expert_ids': expert_ids, 'gate_vals': gate_vals, 'w_gate': w_gate, 'w_up': w_up, 'w_down': w_down}


def expert_ffn(row_in, gate_mat, up_mat, down_mat):
    gate_act = jnp.dot(row_in, gate_mat, preferred_element_type=jnp.float32)
    up_act = jnp.dot(row_in, up_mat, preferred_element_type=jnp.float32)
    hidden = (jax.nn.silu(gate_act) * up_act).astype(jnp.bfloat16)
    return jnp.dot(hidden, down_mat, preferred_element_type=jnp.float32).astype(jnp.bfloat16)


def reference(tokens, expert_ids, gate_vals, w_gate, w_up, w_down):
    pair_count = TOKENS * TOP_K
    flat_ids = expert_ids.reshape(pair_count)
    pair_index = jnp.arange(pair_count, dtype=jnp.int32)

    def one_expert(map_item):
        expert, gate_mat, up_mat, down_mat = map_item
        member = flat_ids == expert
        slot_pos = jnp.where(member, jnp.cumsum(member.astype(jnp.int32)) - 1, EXPERT_CAP)
        pair_list = jnp.full((EXPERT_CAP,), pair_count, jnp.int32).at[slot_pos].set(pair_index, mode='drop')
        row_in = tokens[jnp.minimum(pair_list, pair_count - 1) // TOP_K]
        return pair_list, expert_ffn(row_in, gate_mat, up_mat, down_mat)

    pair_lists, expert_rows = lax.map(one_expert, (jnp.arange(NUM_EXPERTS, dtype=jnp.int32), w_gate, w_up, w_down))
    pair_out = jnp.zeros((pair_count, D_MODEL), jnp.bfloat16).at[pair_lists.reshape(-1)].set(expert_rows.reshape(-1, D_MODEL), mode='drop')
    earlier = jnp.arange(TOP_K)[None, :] < jnp.arange(TOP_K)[:, None]

    def combine_block(blk_item):
        rows_in, ids_in, gate_in, outs_in = blk_item
        dev_of = ids_in // LOCAL_EXPERTS
        same_dev = dev_of[:, :, None] == dev_of[:, None, :]
        weights = jnp.where(same_dev, gate_in[:, None, :], 0.0)
        dev_sum = jnp.einsum('tjk,tkd->tjd', weights, outs_in.astype(jnp.float32)).astype(jnp.bfloat16)
        leader = jnp.logical_not(jnp.any(same_dev & earlier[None, :, :], axis=2))
        moe_sum = jnp.sum(jnp.where(leader[:, :, None], dev_sum.astype(jnp.float32), 0.0), axis=1)
        return (rows_in.astype(jnp.float32) + moe_sum).astype(jnp.bfloat16)

    output = lax.map(combine_block, (tokens.reshape(GROUP, TOK_DEV, D_MODEL), expert_ids.reshape(GROUP, TOK_DEV, TOP_K), gate_vals.reshape(GROUP, TOK_DEV, TOP_K), pair_out.reshape(GROUP, TOK_DEV, TOP_K, D_MODEL)))
    return output.reshape(TOKENS, D_MODEL)
```

```python
import functools

import jax
import jax.numpy as jnp
from jax import lax
from jax.experimental import pallas as pl
from jax.experimental.pallas import tpu as pltpu
from jax.sharding import PartitionSpec as P

MESH = pl.DeviceIdType.MESH
F32, BF16 = jnp.float32, jnp.bfloat16
GROUPS = 4
CAP = 128
KB = 512
DB = 256
RING1 = 8
EPS = 4
RING2 = 4


def layer_kernel(tok, ids_in, gts_in, w_gate, w_up, w_down, out, acc, rows_all, own, hid, ring1, ring2, back, pick1, pick2,
                 y_blk, xbuf, ids_all, gts_all, slots, tbl, w1_sem, w2_sem, loc_sem, idx_send, idx_recv, d_send, d_recv,
                 r_send, r_recv, o_sem):
    tok_dev, d_model = tok.shape
    n_exp, _, ffn = w_gate.shape
    n_tok = GROUPS * tok_dev
    n_kb, n_db, n_grp = d_model // KB, d_model // DB, n_exp // EPS
    steps1, steps2 = n_kb * n_exp, n_db * n_grp

    me = lax.axis_index('ep')
    sib = me + 1 - 2 * lax.rem(me, 2)
    over = lax.rem(me + 2, GROUPS)
    diag = lax.rem(sib + 2, GROUPS)
    peers = (over, diag, sib)

    def rows_of(dev):
        return pl.ds(pl.multiple_of(dev * tok_dev, tok_dev), tok_dev)

    def w1_copies(step, slot):
        e, k = lax.rem(step, n_exp), lax.div(step, n_exp)
        rows = pl.ds(pl.multiple_of(k * KB, KB), KB)
        return (pltpu.make_async_copy(w_gate.at[e, rows, :], ring1.at[slot, 0], w1_sem.at[slot, 0]),
                pltpu.make_async_copy(w_up.at[e, rows, :], ring1.at[slot, 1], w1_sem.at[slot, 1]))

    def w2_copy(step, slot):
        g, d = lax.rem(step, n_grp), lax.div(step, n_grp)
        cols = pl.ds(pl.multiple_of(d * DB, DB), DB)
        return pltpu.make_async_copy(w_down.at[pl.ds(g * EPS, EPS), :, cols], ring2.at[slot], w2_sem.at[slot])

    own_copy = pltpu.make_async_copy(tok, own, loc_sem.at[0])
    mine_copy = pltpu.make_async_copy(tok, rows_all.at[rows_of(me), :], loc_sem.at[1])
    own_copy.start()
    mine_copy.start()

    def prefetch1(step, c):
        for copy in w1_copies(step, step):
            copy.start()
        return c

    lax.fori_loop(0, RING1, prefetch1, 0)

    def prefetch2(step, c):
        w2_copy(step, step).start()
        return c

    lax.fori_loop(0, RING2, prefetch2, 0)

    barrier = pltpu.get_barrier_semaphore()
    for dev in peers:
        pl.semaphore_signal(barrier, inc=1, device_id={'ep': dev}, device_id_type=MESH)
    pl.semaphore_wait(barrier, len(peers))

    def idx_copy(j, what):
        src, dst = (ids_in, ids_all) if what == 0 else (gts_in, gts_all)
        return pltpu.make_async_remote_copy(src_ref=src, dst_ref=dst.at[j], send_sem=idx_send.at[what, j], recv_sem=idx_recv.at[what, j],
                                            device_id={'ep': peers[j]}, device_id_type=MESH)

    def disp_copy(kind, k):
        cols = pl.ds(k * KB, KB) if isinstance(k, int) else pl.ds(pl.multiple_of(k * KB, KB), KB)
        if kind == 2:
            src = dst = rows_all.at[rows_of(over), cols]
        else:
            src, dst = own.at[:, cols], rows_all.at[rows_of(me), cols]
        return pltpu.make_async_remote_copy(src_ref=src, dst_ref=dst, send_sem=d_send.at[kind, k], recv_sem=d_recv.at[kind, k],
                                            device_id={'ep': over if kind == 0 else sib}, device_id_type=MESH)

    def disp_arrival(kind, k):
        cols = pl.ds(pl.multiple_of(k * KB, KB), KB)
        dst = rows_all.at[rows_of((over, sib, diag)[kind]), cols]
        return pltpu.make_async_remote_copy(src_ref=dst, dst_ref=dst, send_sem=d_send.at[kind, k], recv_sem=d_recv.at[kind, k],
                                            device_id={'ep': over if kind == 0 else sib}, device_id_type=MESH)

    for j in range(3):
        for what in range(2):
            idx_copy(j, what).start()
    own_copy.wait()
    for k in range(n_kb):
        disp_copy(0, k).start()
        disp_copy(1, k).start()

    for j in range(3):
        for what in range(2):
            idx_copy(j, what).wait()

    expert = lax.broadcasted_iota(jnp.int32, (n_exp, tok_dev), 0) + me * n_exp

    def side(src, ids_ref, gts_ref):
        ids, gts = ids_ref[...], gts_ref[...]
        hit_any = jnp.zeros((n_exp, tok_dev), jnp.int32)
        gate = jnp.zeros((n_exp, tok_dev), F32)
        for j in range(ids.shape[0]):
            hit = ids[j:j + 1, :] == expert
            hit_any = hit_any + jnp.where(hit, 1, 0)
            gate = gate + jnp.where(hit, gts[j:j + 1, :], 0.0)
        return hit_any, gate

    parts = {'me': side(None, ids_in, gts_in)}
    for j, name in enumerate(('over', 'diag', 'sib')):
        parts[name] = side(None, ids_all.at[j], gts_all.at[j])

    def pick_part(b, i):
        return jnp.where(me == b, parts['me'][i], jnp.where(over == b, parts['over'][i], jnp.where(diag == b, parts['diag'][i], parts['sib'][i])))

    member = jnp.concatenate([pick_part(b, 0) for b in range(GROUPS)], axis=1)
    gate = jnp.concatenate([pick_part(b, 1) for b in range(GROUPS)], axis=1)
    lane = lax.broadcasted_iota(jnp.int32, (n_exp, n_tok), 1)
    count = member
    shift = 1
    while shift < n_tok:
        count = count + jnp.where(lane >= shift, pltpu.roll(count, shift, 1), 0)
        shift *= 2
    is_mem = member > 0
    slot = jnp.where(is_mem, count - 1, -1)
    slots[...] = slot
    pos = lax.broadcasted_iota(jnp.int32, (n_exp, n_tok), 0) * CAP + slot
    big = n_exp * CAP
    pos1 = jnp.min(jnp.where(is_mem, pos, big), axis=0, keepdims=True)
    pos2 = jnp.max(jnp.where(is_mem, pos, -1), axis=0, keepdims=True)
    g1 = jnp.sum(jnp.where(is_mem & (pos == pos1), gate, 0.0), axis=0, keepdims=True)
    g2 = jnp.sum(jnp.where(is_mem & (pos == pos2), gate, 0.0), axis=0, keepdims=True)
    sub = lax.broadcasted_iota(jnp.int32, (8, n_tok), 0)
    packed = jnp.where(sub == 0, pos1.astype(F32), jnp.where(sub == 1, pos2.astype(F32), jnp.where(sub == 2, g1, jnp.where(sub == 3, g2, 0.0))))
    tbl[...] = jnp.transpose(packed)

    def build_picks(i, c):
        r = pl.ds(pl.multiple_of(i * 128, 128), 128)
        at = lax.broadcasted_iota(jnp.int32, (128, big), 1).astype(F32)
        pick1[r, :] = jnp.where(tbl[r, 0:1] == at, 1.0, 0.0).astype(BF16)
        pick2[r, :] = jnp.where(tbl[r, 1:2] == at, 1.0, 0.0).astype(BF16)
        return c

    lax.fori_loop(0, n_tok // 128, build_picks, 0)
    mine_copy.wait()

    def fan(e, k, par):
        cols = pl.ds(k * KB, KB)
        hot = lax.broadcasted_iota(jnp.int32, (CAP, n_tok), 0) == slots[pl.ds(e, 1), :]
        hot = jnp.where(hot, 1.0, 0.0).astype(BF16)
        xbuf[par] = jnp.dot(hot, rows_all[:, cols], preferred_element_type=F32).astype(BF16)

    disp_arrival(0, 0).wait_recv()
    disp_copy(2, 0).start()
    for k in range(n_kb):
        disp_arrival(1, k).wait_recv()
        disp_arrival(2, k).wait_recv()
        fan(0, k, 0)

        def step1(e, c, k=k):
            step = k * n_exp + e
            ring = lax.rem(step, RING1)
            par = lax.rem(e, 2)
            for copy in w1_copies(step, ring):
                copy.wait()
            x = xbuf[par]
            r = pl.ds(pl.multiple_of(e * CAP, CAP), CAP)
            gate_act = jnp.dot(x, ring1[ring, 0], preferred_element_type=F32)
            up_act = jnp.dot(x, ring1[ring, 1], preferred_element_type=F32)
            fan(lax.rem(e + 1, n_exp), k, 1 - par)
            if k > 0:
                gate_act = acc[r, :ffn] + gate_act
                up_act = acc[r, ffn:] + up_act
            if k < n_kb - 1:
                acc[r, :ffn] = gate_act
                acc[r, ffn:] = up_act
            else:
                hid[r, :] = (jax.nn.silu(gate_act) * up_act).astype(BF16)

            @pl.when(step + RING1 < steps1)
            def _():
                for copy in w1_copies(step + RING1, ring):
                    copy.start()

            if k < n_kb - 1:
                @pl.when(e == n_exp - 5)
                def _():
                    disp_arrival(0, k + 1).wait_recv()
                    disp_copy(2, k + 1).start()
            return c

        lax.fori_loop(0, n_exp, step1, 0)

    for k in range(n_kb):
        for kind in range(3):
            disp_copy(kind, k).wait_send()

    def ret_copy(j, d):
        cols = pl.ds(pl.multiple_of(d * DB, DB), DB)
        return pltpu.make_async_remote_copy(src_ref=rows_all.at[rows_of(peers[j]), cols], dst_ref=back.at[j, :, cols],
                                            send_sem=r_send.at[j, d], recv_sem=r_recv.at[j, d], device_id={'ep': peers[j]}, device_id_type=MESH)

    def block2(d, c):
        cols = pl.ds(pl.multiple_of(d * DB, DB), DB)

        def step2(g, c2):
            step = d * n_grp + g
            ring = lax.rem(step, RING2)
            w2_copy(step, ring).wait()
            for i in range(EPS):
                r = pl.ds(pl.multiple_of((g * EPS + i) * CAP, CAP), CAP)
                y_blk[r, :] = jnp.dot(hid[r, :], ring2[ring, i], preferred_element_type=F32).astype(BF16)

            @pl.when(step + RING2 < steps2)
            def _():
                w2_copy(step + RING2, ring).start()
            return c2

        lax.fori_loop(0, n_grp, step2, 0)

        for j, dev in enumerate((*peers, me)):
            r = rows_of(dev)
            y1 = jnp.dot(pick1[r, :], y_blk[...], preferred_element_type=F32)
            y2 = jnp.dot(pick2[r, :], y_blk[...], preferred_element_type=F32)
            rows_all[r, cols] = (tbl[r, 2:3] * y1 + tbl[r, 3:4] * y2).astype(BF16)
            if j < 3:
                ret_copy(j, d).start()
        return c

    lax.fori_loop(0, n_db, block2, 0)

    def out_copy(d):
        cols = pl.ds(pl.multiple_of(d * DB, DB), DB)
        return pltpu.make_async_copy(own.at[:, cols], out.at[:, cols], o_sem.at[d])

    def finish(d, c):
        cols = pl.ds(pl.multiple_of(d * DB, DB), DB)
        for j in range(3):
            ret_copy(j, d).wait_recv()
        total = own[:, cols].astype(F32) + rows_all[rows_of(me), cols].astype(F32)
        for j in range(3):
            total = total + back[j, :, cols].astype(F32)
        own[:, cols] = total.astype(BF16)
        out_copy(d).start()
        return c

    lax.fori_loop(0, n_db, finish, 0)

    def drain(d, c):
        for j in range(3):
            ret_copy(j, d).wait_send()
        out_copy(d).wait()
        return c

    lax.fori_loop(0, n_db, drain, 0)


def solution(mesh):
    row_spec = P(('dp', 'ep'))
    expert_spec = P('ep')

    def device_step(tokens, expert_ids, gate_vals, w_gate, w_up, w_down):
        tok_dev, d_model = tokens.shape
        n_exp, _, ffn = w_gate.shape
        top_k = expert_ids.shape[1]
        n_tok = GROUPS * tok_dev
        pairs = n_exp * CAP
        hbm = pl.BlockSpec(memory_space=pltpu.HBM)
        vmem = pl.BlockSpec(memory_space=pltpu.VMEM)
        dma = pltpu.SemaphoreType.DMA
        return pl.pallas_call(
            layer_kernel,
            out_shape=jax.ShapeDtypeStruct((tok_dev, d_model), BF16),
            in_specs=[hbm, vmem, vmem, hbm, hbm, hbm],
            out_specs=hbm,
            scratch_shapes=[
                pltpu.VMEM((pairs, 2 * ffn), F32),
                pltpu.VMEM((n_tok, d_model), BF16),
                pltpu.VMEM((tok_dev, d_model), BF16),
                pltpu.VMEM((pairs, ffn), BF16),
                pltpu.VMEM((RING1, 2, KB, ffn), BF16),
                pltpu.VMEM((RING2, EPS, ffn, DB), BF16),
                pltpu.VMEM((3, tok_dev, d_model), BF16),
                pltpu.VMEM((n_tok, pairs), BF16),
                pltpu.VMEM((n_tok, pairs), BF16),
                pltpu.VMEM((pairs, DB), BF16),
                pltpu.VMEM((2, CAP, KB), BF16),
                pltpu.VMEM((3, top_k, tok_dev), jnp.int32),
                pltpu.VMEM((3, top_k, tok_dev), F32),
                pltpu.VMEM((n_exp, n_tok), jnp.int32),
                pltpu.VMEM((n_tok, 8), F32),
                dma((RING1, 2)),
                dma((RING2,)),
                dma((2,)),
                dma((2, 3)),
                dma((2, 3)),
                dma((3, d_model // KB)),
                dma((3, d_model // KB)),
                dma((3, d_model // DB)),
                dma((3, d_model // DB)),
                dma((d_model // DB,)),
            ],
            compiler_params=pltpu.CompilerParams(collective_id=0, has_side_effects=True, vmem_limit_bytes=67043328),
        )(tokens, expert_ids.T, gate_vals.T, w_gate, w_up, w_down)

    return jax.shard_map(device_step, mesh=mesh, in_specs=(row_spec, row_spec, row_spec, expert_spec, expert_spec, expert_spec), out_specs=row_spec, check_vma=False)
```

```python
import functools

import jax
import jax.numpy as jnp
from jax import lax
from jax.experimental import pallas as pl
from jax.experimental.pallas import tpu as pltpu
from jax.sharding import PartitionSpec as P

MESH = pl.DeviceIdType.MESH
F32, BF16 = jnp.float32, jnp.bfloat16
GROUPS = 4
CAP = 128
KU = 256
BLOCKS = (1, 1, 2, 2, 2)
DB = 256
RING1 = 8
PER_BODY = 2
EPS = 4
RING2 = 4


def layer_kernel(tok, ids_in, gts_in, w_gate, w_up, w_down, out, acc, rows_all, own, hid, ring1, ring2, back, pick1, pick2,
                 y_blk, xbuf1, xbuf2, ids_all, gts_all, slots, tbl, w1_sem, w2_sem, loc_sem, idx_send, idx_recv, d_send, d_recv,
                 r_send, r_recv, o_sem):
    tok_dev, d_model = tok.shape
    n_exp, n_unit, _, ffn = w_gate.shape
    n_tok = GROUPS * tok_dev
    n_kb, n_db, n_grp = len(BLOCKS), d_model // DB, n_exp // EPS
    firsts = [sum(BLOCKS[:k]) for k in range(n_kb)]
    assert sum(BLOCKS) == n_unit
    slot_exp = [2 // width for width in BLOCKS]
    body_exp = [PER_BODY * m for m in slot_exp]
    bodies = [n_exp // m for m in body_exp]
    xbufs = {1: xbuf1, 2: xbuf2}
    steps2 = n_db * n_grp

    me = lax.axis_index('ep')
    sib = me + 1 - 2 * lax.rem(me, 2)
    over = lax.rem(me + 2, GROUPS)
    diag = lax.rem(sib + 2, GROUPS)
    peers = (over, diag, sib)

    def rows_of(dev):
        return pl.ds(pl.multiple_of(dev * tok_dev, tok_dev), tok_dev)

    def w1_copies(k, i, slot):
        if BLOCKS[k] == 2:
            part = (i, pl.ds(firsts[k], 2))
        else:
            part = (pl.ds(i * 2, 2), firsts[k])
        return (pltpu.make_async_copy(w_gate.at[part], ring1.at[slot, 0], w1_sem.at[slot, 0]),
                pltpu.make_async_copy(w_up.at[part], ring1.at[slot, 1], w1_sem.at[slot, 1]))

    def w2_copy(step, slot):
        g, d = lax.rem(step, n_grp), lax.div(step, n_grp)
        cols = pl.ds(pl.multiple_of(d * DB, DB), DB)
        return pltpu.make_async_copy(w_down.at[pl.ds(g * EPS, EPS), :, cols], ring2.at[slot], w2_sem.at[slot])

    own_copy = pltpu.make_async_copy(tok, own, loc_sem.at[0])
    mine_copy = pltpu.make_async_copy(tok, rows_all.at[rows_of(me), :], loc_sem.at[1])
    own_copy.start()
    mine_copy.start()

    def prefetch1(step, c):
        for copy in w1_copies(0, step, step):
            copy.start()
        return c

    lax.fori_loop(0, RING1, prefetch1, 0)

    def prefetch2(step, c):
        w2_copy(step, step).start()
        return c

    lax.fori_loop(0, RING2, prefetch2, 0)

    barrier = pltpu.get_barrier_semaphore()
    for dev in peers:
        pl.semaphore_signal(barrier, inc=1, device_id={'ep': dev}, device_id_type=MESH)
    pl.semaphore_wait(barrier, len(peers))

    def idx_copy(j, what):
        src, dst = (ids_in, ids_all) if what == 0 else (gts_in, gts_all)
        return pltpu.make_async_remote_copy(src_ref=src, dst_ref=dst.at[j], send_sem=idx_send.at[what, j], recv_sem=idx_recv.at[what, j],
                                            device_id={'ep': peers[j]}, device_id_type=MESH)

    def disp_copy(kind, k):
        cols = pl.ds(firsts[k] * KU, BLOCKS[k] * KU)
        if kind == 2:
            src = dst = rows_all.at[rows_of(over), cols]
        else:
            src, dst = own.at[:, cols], rows_all.at[rows_of(me), cols]
        return pltpu.make_async_remote_copy(src_ref=src, dst_ref=dst, send_sem=d_send.at[kind, k], recv_sem=d_recv.at[kind, k],
                                            device_id={'ep': over if kind == 0 else sib}, device_id_type=MESH)

    def disp_arrival(kind, k):
        cols = pl.ds(firsts[k] * KU, BLOCKS[k] * KU)
        dst = rows_all.at[rows_of((over, sib, diag)[kind]), cols]
        return pltpu.make_async_remote_copy(src_ref=dst, dst_ref=dst, send_sem=d_send.at[kind, k], recv_sem=d_recv.at[kind, k],
                                            device_id={'ep': over if kind == 0 else sib}, device_id_type=MESH)

    for j in range(3):
        for what in range(2):
            idx_copy(j, what).start()
    own_copy.wait()
    for k in range(n_kb):
        disp_copy(0, k).start()
        disp_copy(1, k).start()

    for j in range(3):
        for what in range(2):
            idx_copy(j, what).wait()

    expert = lax.broadcasted_iota(jnp.int32, (n_exp, tok_dev), 0) + me * n_exp

    def side(src, ids_ref, gts_ref):
        ids, gts = ids_ref[...], gts_ref[...]
        hit_any = jnp.zeros((n_exp, tok_dev), jnp.int32)
        gate = jnp.zeros((n_exp, tok_dev), F32)
        for j in range(ids.shape[0]):
            hit = ids[j:j + 1, :] == expert
            hit_any = hit_any + jnp.where(hit, 1, 0)
            gate = gate + jnp.where(hit, gts[j:j + 1, :], 0.0)
        return hit_any, gate

    parts = {'me': side(None, ids_in, gts_in)}
    for j, name in enumerate(('over', 'diag', 'sib')):
        parts[name] = side(None, ids_all.at[j], gts_all.at[j])

    def pick_part(b, i):
        return jnp.where(me == b, parts['me'][i], jnp.where(over == b, parts['over'][i], jnp.where(diag == b, parts['diag'][i], parts['sib'][i])))

    member = jnp.concatenate([pick_part(b, 0) for b in range(GROUPS)], axis=1)
    gate = jnp.concatenate([pick_part(b, 1) for b in range(GROUPS)], axis=1)
    lane = lax.broadcasted_iota(jnp.int32, (n_exp, n_tok), 1)
    count = member
    shift = 1
    while shift < n_tok:
        count = count + jnp.where(lane >= shift, pltpu.roll(count, shift, 1), 0)
        shift *= 2
    is_mem = member > 0
    slot = jnp.where(is_mem, count - 1, -1)
    slots[...] = slot
    pos = lax.broadcasted_iota(jnp.int32, (n_exp, n_tok), 0) * CAP + slot
    big = n_exp * CAP
    pos1 = jnp.min(jnp.where(is_mem, pos, big), axis=0, keepdims=True)
    pos2 = jnp.max(jnp.where(is_mem, pos, -1), axis=0, keepdims=True)
    g1 = jnp.sum(jnp.where(is_mem & (pos == pos1), gate, 0.0), axis=0, keepdims=True)
    g2 = jnp.sum(jnp.where(is_mem & (pos == pos2), gate, 0.0), axis=0, keepdims=True)
    sub = lax.broadcasted_iota(jnp.int32, (8, n_tok), 0)
    packed = jnp.where(sub == 0, pos1.astype(F32), jnp.where(sub == 1, pos2.astype(F32), jnp.where(sub == 2, g1, jnp.where(sub == 3, g2, 0.0))))
    tbl[...] = jnp.transpose(packed)

    def build_picks(i, c):
        r = pl.ds(pl.multiple_of(i * 128, 128), 128)
        at = lax.broadcasted_iota(jnp.int32, (128, big), 1).astype(F32)
        pick1[r, :] = jnp.where(tbl[r, 0:1] == at, 1.0, 0.0).astype(BF16)
        pick2[r, :] = jnp.where(tbl[r, 1:2] == at, 1.0, 0.0).astype(BF16)
        return c

    lax.fori_loop(0, n_tok // 128, build_picks, 0)
    mine_copy.wait()

    def fan(k, i, par):
        cols = pl.ds(firsts[k] * KU, BLOCKS[k] * KU)
        at = lax.broadcasted_iota(jnp.int32, (CAP, n_tok), 0)
        hot = jnp.concatenate([jnp.where(at == slots[pl.ds(i * body_exp[k] + m, 1), :], 1.0, 0.0).astype(BF16) for m in range(body_exp[k])], axis=0)
        xbufs[BLOCKS[k]][par] = jnp.dot(hot, rows_all[:, cols], preferred_element_type=F32).astype(BF16)

    def body1(k, i, nxt):
        par = lax.rem(i, 2) if not isinstance(i, int) else i % 2
        base = sum(n_exp // slot_exp[j] for j in range(k)) + i * PER_BODY
        rings = [lax.rem(base + m, RING1) if not isinstance(i, int) else (base + m) % RING1 for m in range(PER_BODY)]
        for m in range(PER_BODY):
            for copy in w1_copies(k, i * PER_BODY + m, rings[m]):
                copy.wait()
        x = xbufs[BLOCKS[k]].at[par]
        for m in range(body_exp[k]):
            ring, xr = rings[m // slot_exp[k]], pl.ds(m * CAP, CAP)
            r = pl.ds(pl.multiple_of((i * body_exp[k] + m) * CAP, CAP), CAP)
            acts = []
            for p in range(2):
                if BLOCKS[k] == 2:
                    act = (jnp.dot(x[xr, :KU], ring1[ring, p, 0], preferred_element_type=F32) +
                           jnp.dot(x[xr, KU:], ring1[ring, p, 1], preferred_element_type=F32))
                else:
                    act = jnp.dot(x[xr, :], ring1[ring, p, m % 2], preferred_element_type=F32)
                if k > 0:
                    act = acc[r, p * ffn:(p + 1) * ffn] + act
                if k < n_kb - 1:
                    acc[r, p * ffn:(p + 1) * ffn] = act
                acts.append(act)
            if k == n_kb - 1:
                hid[r, :] = (jax.nn.silu(acts[0]) * acts[1]).astype(BF16)
        if nxt is not None:
            fan(*nxt, 1 - par)

        for m in range(PER_BODY):
            ahead, n_here = i * PER_BODY + m + RING1, n_exp // slot_exp[k]

            def refill(kk, ii, m=m):
                for copy in w1_copies(kk, ii, rings[m]):
                    copy.start()

            if isinstance(i, int):
                if ahead < n_here:
                    refill(k, ahead)
                elif k < n_kb - 1:
                    refill(k + 1, ahead - n_here)
            elif n_here == RING1:
                refill(k + 1, ahead - n_here)
            else:
                @pl.when(ahead < n_here)
                def _():
                    refill(k, ahead)

                if k < n_kb - 1:
                    @pl.when(ahead >= n_here)
                    def _():
                        refill(k + 1, ahead - n_here)

    disp_arrival(0, 0).wait_recv()
    disp_copy(2, 0).start()
    disp_arrival(1, 0).wait_recv()
    disp_arrival(2, 0).wait_recv()
    fan(0, 0, 0)
    for k in range(n_kb):
        def loop1(i, c, k=k):
            body1(k, i, (k, i + 1))
            if k < n_kb - 1:
                @pl.when(i == bodies[k] - 3)
                def _():
                    disp_arrival(0, k + 1).wait_recv()
                    disp_copy(2, k + 1).start()
            return c

        lax.fori_loop(0, bodies[k] - 1, loop1, 0)
        if k < n_kb - 1:
            disp_arrival(1, k + 1).wait_recv()
            disp_arrival(2, k + 1).wait_recv()
        body1(k, bodies[k] - 1, (k + 1, 0) if k < n_kb - 1 else None)

    for k in range(n_kb):
        for kind in range(3):
            disp_copy(kind, k).wait_send()

    def ret_copy(j, d):
        cols = pl.ds(pl.multiple_of(d * DB, DB), DB)
        return pltpu.make_async_remote_copy(src_ref=rows_all.at[rows_of(peers[j]), cols], dst_ref=back.at[j, :, cols],
                                            send_sem=r_send.at[j, d], recv_sem=r_recv.at[j, d], device_id={'ep': peers[j]}, device_id_type=MESH)

    def block2(d, c):
        cols = pl.ds(pl.multiple_of(d * DB, DB), DB)

        def step2(g, c2):
            step = d * n_grp + g
            ring = lax.rem(step, RING2)
            w2_copy(step, ring).wait()
            for i in range(EPS):
                r = pl.ds(pl.multiple_of((g * EPS + i) * CAP, CAP), CAP)
                y_blk[r, :] = jnp.dot(hid[r, :], ring2[ring, i], preferred_element_type=F32).astype(BF16)

            @pl.when(step + RING2 < steps2)
            def _():
                w2_copy(step + RING2, ring).start()
            return c2

        lax.fori_loop(0, n_grp, step2, 0)

        for j, dev in enumerate((*peers, me)):
            r = rows_of(dev)
            y1 = jnp.dot(pick1[r, :], y_blk[...], preferred_element_type=F32)
            y2 = jnp.dot(pick2[r, :], y_blk[...], preferred_element_type=F32)
            rows_all[r, cols] = (tbl[r, 2:3] * y1 + tbl[r, 3:4] * y2).astype(BF16)
            if j < 3:
                ret_copy(j, d).start()
        return c

    lax.fori_loop(0, n_db, block2, 0)

    def out_copy(d):
        cols = pl.ds(pl.multiple_of(d * DB, DB), DB)
        return pltpu.make_async_copy(own.at[:, cols], out.at[:, cols], o_sem.at[d])

    def finish(d, c):
        cols = pl.ds(pl.multiple_of(d * DB, DB), DB)
        for j in range(3):
            ret_copy(j, d).wait_recv()
        total = own[:, cols].astype(F32) + rows_all[rows_of(me), cols].astype(F32)
        for j in range(3):
            total = total + back[j, :, cols].astype(F32)
        own[:, cols] = total.astype(BF16)
        out_copy(d).start()
        return c

    lax.fori_loop(0, n_db, finish, 0)

    def drain(d, c):
        for j in range(3):
            ret_copy(j, d).wait_send()
        out_copy(d).wait()
        return c

    lax.fori_loop(0, n_db, drain, 0)


def solution(mesh):
    row_spec = P(('dp', 'ep'))
    expert_spec = P('ep')

    def device_step(tokens, expert_ids, gate_vals, w_gate, w_up, w_down):
        tok_dev, d_model = tokens.shape
        n_exp, _, ffn = w_gate.shape
        top_k = expert_ids.shape[1]
        n_tok = GROUPS * tok_dev
        pairs = n_exp * CAP
        units = (n_exp, d_model // KU, KU, ffn)
        hbm = pl.BlockSpec(memory_space=pltpu.HBM)
        vmem = pl.BlockSpec(memory_space=pltpu.VMEM)
        dma = pltpu.SemaphoreType.DMA
        return pl.pallas_call(
            layer_kernel,
            out_shape=jax.ShapeDtypeStruct((tok_dev, d_model), BF16),
            in_specs=[hbm, vmem, vmem, hbm, hbm, hbm],
            out_specs=hbm,
            scratch_shapes=[
                pltpu.VMEM((pairs, 2 * ffn), F32),
                pltpu.VMEM((n_tok, d_model), BF16),
                pltpu.VMEM((tok_dev, d_model), BF16),
                pltpu.VMEM((pairs, ffn), BF16),
                pltpu.VMEM((RING1, 2, 2, KU, ffn), BF16),
                pltpu.VMEM((RING2, EPS, ffn, DB), BF16),
                pltpu.VMEM((3, tok_dev, d_model), BF16),
                pltpu.VMEM((n_tok, pairs), BF16),
                pltpu.VMEM((n_tok, pairs), BF16),
                pltpu.VMEM((pairs, DB), BF16),
                pltpu.VMEM((2, 4 * CAP, KU), BF16),
                pltpu.VMEM((2, 2 * CAP, 2 * KU), BF16),
                pltpu.VMEM((3, top_k, tok_dev), jnp.int32),
                pltpu.VMEM((3, top_k, tok_dev), F32),
                pltpu.VMEM((n_exp, n_tok), jnp.int32),
                pltpu.VMEM((n_tok, 8), F32),
                dma((RING1, 2)),
                dma((RING2,)),
                dma((2,)),
                dma((2, 3)),
                dma((2, 3)),
                dma((3, len(BLOCKS))),
                dma((3, len(BLOCKS))),
                dma((3, d_model // DB)),
                dma((3, d_model // DB)),
                dma((d_model // DB,)),
            ],
            compiler_params=pltpu.CompilerParams(collective_id=0, has_side_effects=True, vmem_limit_bytes=67043328),
        )(tokens, expert_ids.T, gate_vals.T, w_gate.reshape(units), w_up.reshape(units), w_down)

    return jax.shard_map(device_step, mesh=mesh, in_specs=(row_spec, row_spec, row_spec, expert_spec, expert_spec, expert_spec), out_specs=row_spec, check_vma=False)
```

```python
import jax
import jax.numpy as jnp
from jax import lax
from jax.experimental import pallas as pl
from jax.experimental.pallas import tpu as pltpu
from jax.sharding import PartitionSpec as P

MESH = pl.DeviceIdType.MESH
F32, BF16 = jnp.float32, jnp.bfloat16
GROUPS = 4
CAP = 128
KU = 256
BLOCKS = (1, 1, 2, 2, 2)
DB = 256
RING1 = 8
EXTRA = 4
PER_BODY = 2
EPS = 4
RING2 = 4


def layer_kernel(tok, ids_in, gts_in, w_gate, w_up, w_down, out, acc, rows_all, own, hid, ring1, ring2, back,
                 y_blk, xbuf, ids_all, gts_all, slots, tbl, w1_sem, w2_sem, loc_sem, idx_send, idx_recv, d_send, d_recv,
                 r_send, r_recv, o_sem):
    tok_dev, d_model = tok.shape
    n_exp, n_unit, _, ffn = w_gate.shape
    n_tok = GROUPS * tok_dev
    n_kb, n_db, n_grp = len(BLOCKS), d_model // DB, n_exp // EPS
    firsts = [sum(BLOCKS[:k]) for k in range(n_kb)]
    assert sum(BLOCKS) == n_unit and BLOCKS[:3] == (1, 1, 2) and set(BLOCKS[2:]) == {2} and n_exp == GROUPS * EPS
    slot_exp = [2 // width for width in BLOCKS]
    body_exp = [PER_BODY * m for m in slot_exp]
    bodies = [n_exp // m for m in body_exp]
    bases = [sum(n_exp // m for m in slot_exp[:k]) for k in range(n_kb + 1)]
    steps2 = n_db * n_grp

    me = lax.axis_index('ep')
    sib = me + 1 - 2 * lax.rem(me, 2)
    over = lax.rem(me + 2, GROUPS)
    diag = lax.rem(sib + 2, GROUPS)
    peers = (over, diag, sib)

    def rows_of(dev):
        return pl.ds(pl.multiple_of(dev * tok_dev, tok_dev), tok_dev)

    def w1_copies(k, i, slot):
        if BLOCKS[k] == 2:
            part = (i, pl.ds(firsts[k], 2))
        else:
            part = (pl.ds(i * 2, 2), firsts[k])
        return (pltpu.make_async_copy(w_gate.at[part], ring1.at[slot, 0], w1_sem.at[slot, 0]),
                pltpu.make_async_copy(w_up.at[part], ring1.at[slot, 1], w1_sem.at[slot, 1]))

    def ring_slot(k, s):
        if k == 0:
            return s
        if k == 1:
            return s % (RING1 + EXTRA)
        return lax.rem(s + RING1 - EXTRA, RING1) if not isinstance(s, int) else (s + RING1 - EXTRA) % RING1

    def w2_copy(step, slot):
        g, d = lax.rem(step, n_grp), lax.div(step, n_grp)
        cols = pl.ds(pl.multiple_of(d * DB, DB), DB)
        return pltpu.make_async_copy(w_down.at[pl.ds(g * EPS, EPS), :, cols], ring2.at[slot], w2_sem.at[slot])

    own_copy = pltpu.make_async_copy(tok, own, loc_sem.at[0])
    mine_copy = pltpu.make_async_copy(tok, rows_all.at[rows_of(me), :], loc_sem.at[1])
    own_copy.start()
    barrier = pltpu.get_barrier_semaphore()
    for dev in peers:
        pl.semaphore_signal(barrier, inc=1, device_id={'ep': dev}, device_id_type=MESH)
    mine_copy.start()
    for s in range(RING1):
        for copy in w1_copies(0, s, s):
            copy.start()
    pl.semaphore_wait(barrier, len(peers))

    def idx_copy(j, what):
        src, dst = (ids_in, ids_all) if what == 0 else (gts_in, gts_all)
        return pltpu.make_async_remote_copy(src_ref=src, dst_ref=dst.at[j], send_sem=idx_send.at[what, j], recv_sem=idx_recv.at[what, j],
                                            device_id={'ep': peers[j]}, device_id_type=MESH)

    def disp_copy(kind, k):
        cols = pl.ds(firsts[k] * KU, BLOCKS[k] * KU)
        if kind == 2:
            src = dst = rows_all.at[rows_of(over), cols]
        else:
            src, dst = own.at[:, cols], rows_all.at[rows_of(me), cols]
        return pltpu.make_async_remote_copy(src_ref=src, dst_ref=dst, send_sem=d_send.at[kind, k], recv_sem=d_recv.at[kind, k],
                                            device_id={'ep': over if kind == 0 else sib}, device_id_type=MESH)

    def disp_arrival(kind, k):
        cols = pl.ds(firsts[k] * KU, BLOCKS[k] * KU)
        dst = rows_all.at[rows_of((over, sib, diag)[kind]), cols]
        return pltpu.make_async_remote_copy(src_ref=dst, dst_ref=dst, send_sem=d_send.at[kind, k], recv_sem=d_recv.at[kind, k],
                                            device_id={'ep': over if kind == 0 else sib}, device_id_type=MESH)

    for j in range(3):
        for what in range(2):
            idx_copy(j, what).start()
    own_copy.wait()
    for k in range(n_kb):
        disp_copy(0, k).start()
        disp_copy(1, k).start()
    for s in range(EXTRA):
        for copy in w1_copies(1, s, RING1 + s):
            copy.start()
    for s in range(RING2):
        w2_copy(s, s).start()

    for j in range(3):
        for what in range(2):
            idx_copy(j, what).wait()

    expert = lax.broadcasted_iota(jnp.int32, (n_exp, tok_dev), 0) + me * n_exp

    def side(ids_ref, gts_ref):
        ids, gts = ids_ref[...], gts_ref[...]
        hit_any = jnp.zeros((n_exp, tok_dev), jnp.int32)
        gate = jnp.zeros((n_exp, tok_dev), F32)
        for j in range(ids.shape[0]):
            hit = ids[j:j + 1, :] == expert
            hit_any = hit_any + jnp.where(hit, 1, 0)
            gate = gate + jnp.where(hit, gts[j:j + 1, :], 0.0)
        return hit_any, gate

    parts = [side(ids_in, gts_in)] + [side(ids_all.at[j], gts_all.at[j]) for j in range(3)]

    def of_device(b, i):
        p = [part[i] for part in parts]
        return jnp.where(me == b, p[0], jnp.where(over == b, p[1], jnp.where(diag == b, p[2], p[3])))

    member = jnp.concatenate([of_device(b, 0) for b in range(GROUPS)], axis=1)
    gate = jnp.concatenate([of_device(b, 1) for b in range(GROUPS)], axis=1)
    lane = lax.broadcasted_iota(jnp.int32, (n_exp, n_tok), 1)
    count = member
    shift = 1
    while shift < n_tok:
        count = count + jnp.where(lane >= shift, pltpu.roll(count, shift, 1), 0)
        shift *= 2
    is_mem = member > 0
    slot = jnp.where(is_mem, count - 1, -1)
    slots[...] = slot
    pos = lax.broadcasted_iota(jnp.int32, (n_exp, n_tok), 0) * CAP + slot
    big = n_exp * CAP
    pos1 = jnp.min(jnp.where(is_mem, pos, big), axis=0, keepdims=True)
    pos2 = jnp.max(jnp.where(is_mem, pos, -1), axis=0, keepdims=True)
    g1 = jnp.sum(jnp.where(is_mem & (pos == pos1), gate, 0.0), axis=0, keepdims=True)
    g2 = jnp.sum(jnp.where(is_mem & (pos == pos2), gate, 0.0), axis=0, keepdims=True)
    sub = lax.broadcasted_iota(jnp.int32, (8, n_tok), 0)
    packed = jnp.where(sub == 0, pos1.astype(F32), jnp.where(sub == 1, pos2.astype(F32), jnp.where(sub == 2, g1, jnp.where(sub == 3, g2, 0.0))))
    tbl[...] = jnp.transpose(packed)
    mine_copy.wait()

    half = big // 2
    pick_rows = n_tok // 8

    def build_picks(i):
        dev, r = i // 2, (i % 2) * pick_rows
        if not isinstance(i, int):
            dev, r = lax.div(i, 2), pl.multiple_of(lax.rem(i, 2) * pick_rows, pick_rows)
        t = tbl[pl.ds(i * pick_rows, pick_rows), :]
        for h in range(2):
            at = (lax.broadcasted_iota(jnp.int32, (pick_rows, half), 1) + h * half).astype(F32)
            for p in range(2):
                ring1[RING1 + dev, h, p, pl.ds(r, pick_rows), :] = jnp.where(t[:, p:p + 1] == at, 1.0, 0.0).astype(BF16)

    def fan(k, i, par):
        cols = pl.ds(firsts[k] * KU, BLOCKS[k] * KU)
        at = lax.broadcasted_iota(jnp.int32, (CAP, n_tok), 0)
        hot = jnp.concatenate([jnp.where(at == slots[pl.ds(i * body_exp[k] + m, 1), :], 1.0, 0.0).astype(BF16) for m in range(body_exp[k])], axis=0)
        x = jnp.dot(hot, rows_all[:, cols], preferred_element_type=F32).astype(BF16)
        for u in range(2):
            if BLOCKS[k] == 2:
                xbuf[par, u] = x[:, u * KU:(u + 1) * KU]
            else:
                xbuf[par, u] = x[u * 2 * CAP:(u + 1) * 2 * CAP, :]

    def down(e, ring):
        r = pl.ds(pl.multiple_of(e * CAP, CAP), CAP)
        y_blk[r, :] = jnp.dot(hid[r, :], ring2[ring, e % EPS if isinstance(e, int) else lax.rem(e, EPS)], preferred_element_type=F32).astype(BF16)

    def body1(k, i, nxt, last_of=None):
        static = isinstance(i, int)
        par = i % 2 if static else lax.rem(i, 2)
        steps = [bases[k] + i * PER_BODY + m for m in range(PER_BODY)]
        rings = [ring_slot(k, s) for s in steps]
        for m in range(PER_BODY):
            for copy in w1_copies(k, i * PER_BODY + m, rings[m]):
                copy.wait()
        for m in range(body_exp[k]):
            ring = rings[m // slot_exp[k]]
            r = pl.ds(pl.multiple_of((i * body_exp[k] + m) * CAP, CAP), CAP)
            acts = []
            for p in range(2):
                if BLOCKS[k] == 2:
                    xr = pl.ds(m * CAP, CAP)
                    act = (jnp.dot(xbuf[par, 0, xr, :], ring1[ring, p, 0], preferred_element_type=F32) +
                           jnp.dot(xbuf[par, 1, xr, :], ring1[ring, p, 1], preferred_element_type=F32))
                else:
                    act = jnp.dot(xbuf[par, m // 2, pl.ds((m % 2) * CAP, CAP), :], ring1[ring, p, m % 2], preferred_element_type=F32)
                if k > 0:
                    act = acc[r, p * ffn:(p + 1) * ffn] + act
                if k < n_kb - 1:
                    acc[r, p * ffn:(p + 1) * ffn] = act
                acts.append(act)
            if k == n_kb - 1:
                hid[r, :] = (jax.nn.silu(acts[0]) * acts[1]).astype(BF16)
        if nxt is not None:
            fan(*nxt, 1 - par)
        if k == 2:
            build_picks(i)
        if last_of is not None:
            for m in range(body_exp[k]):
                e = last_of * body_exp[k] + m
                down(e, e // EPS if isinstance(e, int) else lax.div(e, EPS))

        for m in range(PER_BODY):
            def refill(s):
                kk = max(j for j in range(n_kb) if bases[j] <= s)
                for copy in w1_copies(kk, s - bases[kk], rings[m]):
                    copy.start()

            if static:
                ahead = steps[m] + RING1 + (EXTRA if steps[m] < RING1 else 0)
                if ahead < bases[n_kb] and not RING1 <= steps[m] < RING1 + EXTRA:
                    refill(ahead)
            else:
                ii, n_here = i * PER_BODY + m + RING1, n_exp // slot_exp[k]

                @pl.when(ii < n_here)
                def _():
                    for copy in w1_copies(k, ii, rings[m]):
                        copy.start()

                if k < n_kb - 1:
                    @pl.when(ii >= n_here)
                    def _():
                        for copy in w1_copies(k + 1, ii - n_here, rings[m]):
                            copy.start()

    disp_arrival(0, 0).wait_recv()
    disp_copy(2, 0).start()
    disp_arrival(1, 0).wait_recv()
    disp_arrival(2, 0).wait_recv()
    fan(0, 0, 0)
    for k in range(n_kb):
        last, n_body = k == n_kb - 1, bodies[k]

        def hand_on(k=k):
            disp_arrival(0, k + 1).wait_recv()
            disp_copy(2, k + 1).start()

        def loop1(i, c, k=k, last=last, n_body=n_body, hand_on=hand_on):
            body1(k, i, (k, i + 1), i - 1 if last else None)
            if not last:
                pl.when(i == n_body - 3)(hand_on)
            return c

        if k < 2:
            for i in range(n_body - 1):
                body1(k, i, (k, i + 1))
                if i == n_body - 3:
                    hand_on()
        elif last:
            for g in range(RING2):
                w2_copy(g, g).wait()
            body1(k, 0, (k, 1))
            lax.fori_loop(1, n_body - 1, loop1, 0)
        else:
            lax.fori_loop(0, n_body - 1, loop1, 0)
        if not last:
            disp_arrival(1, k + 1).wait_recv()
            disp_arrival(2, k + 1).wait_recv()
        body1(k, n_body - 1, None if last else (k + 1, 0), n_body - 2 if last else None)

    for m in range(body_exp[-1]):
        down(n_exp - body_exp[-1] + m, n_grp - 1)

    def refill2(g, c):
        w2_copy(n_grp + g, g).start()
        return c

    lax.fori_loop(0, RING2, refill2, 0)

    for k in range(n_kb):
        for kind in range(3):
            disp_copy(kind, k).wait_send()

    def ret_copy(j, d):
        cols = pl.ds(pl.multiple_of(d * DB, DB), DB)
        return pltpu.make_async_remote_copy(src_ref=rows_all.at[rows_of(peers[j]), cols], dst_ref=back.at[j, :, cols],
                                            send_sem=r_send.at[j, d], recv_sem=r_recv.at[j, d], device_id={'ep': peers[j]}, device_id_type=MESH)

    def combine(d):
        cols = pl.ds(pl.multiple_of(d * DB, DB), DB)
        for j, dev in enumerate((*peers, me)):
            r = rows_of(dev)
            y12 = sum(jnp.dot(ring1[RING1 + dev, h].reshape(2 * tok_dev, half), y_blk[h * half:(h + 1) * half, :], preferred_element_type=F32) for h in range(2))
            rows_all[r, cols] = (tbl[r, 2:3] * y12[:tok_dev] + tbl[r, 3:4] * y12[tok_dev:]).astype(BF16)
            if j < 3:
                ret_copy(j, d).start()

    combine(0)

    def block2(d, c):
        def step2(g, c2):
            step = d * n_grp + g
            ring = lax.rem(step, RING2)
            w2_copy(step, ring).wait()
            for i in range(EPS):
                r = pl.ds(pl.multiple_of((g * EPS + i) * CAP, CAP), CAP)
                y_blk[r, :] = jnp.dot(hid[r, :], ring2[ring, i], preferred_element_type=F32).astype(BF16)

            @pl.when(step + RING2 < steps2)
            def _():
                w2_copy(step + RING2, ring).start()
            return c2

        lax.fori_loop(0, n_grp, step2, 0)
        combine(d)
        return c

    lax.fori_loop(1, n_db, block2, 0)

    def out_copy(d):
        cols = pl.ds(pl.multiple_of(d * DB, DB), DB)
        return pltpu.make_async_copy(own.at[:, cols], out.at[:, cols], o_sem.at[d])

    def finish(d, c):
        cols = pl.ds(pl.multiple_of(d * DB, DB), DB)
        for j in range(3):
            ret_copy(j, d).wait_recv()
        total = own[:, cols].astype(F32) + rows_all[rows_of(me), cols].astype(F32)
        for j in range(3):
            total = total + back[j, :, cols].astype(F32)
        own[:, cols] = total.astype(BF16)
        out_copy(d).start()
        return c

    lax.fori_loop(0, n_db, finish, 0)

    def drain(d, c):
        for j in range(3):
            ret_copy(j, d).wait_send()
        out_copy(d).wait()
        return c

    lax.fori_loop(0, n_db, drain, 0)


def solution(mesh):
    row_spec = P(('dp', 'ep'))
    expert_spec = P('ep')

    def device_step(tokens, expert_ids, gate_vals, w_gate, w_up, w_down):
        tok_dev, d_model = tokens.shape
        n_exp, _, ffn = w_gate.shape
        top_k = expert_ids.shape[1]
        n_tok = GROUPS * tok_dev
        pairs = n_exp * CAP
        units = (n_exp, d_model // KU, KU, ffn)
        hbm = pl.BlockSpec(memory_space=pltpu.HBM)
        vmem = pl.BlockSpec(memory_space=pltpu.VMEM)
        dma = pltpu.SemaphoreType.DMA
        return pl.pallas_call(
            layer_kernel,
            out_shape=jax.ShapeDtypeStruct((tok_dev, d_model), BF16),
            in_specs=[hbm, vmem, vmem, hbm, hbm, hbm],
            out_specs=hbm,
            scratch_shapes=[
                pltpu.VMEM((pairs, 2 * ffn), F32),
                pltpu.VMEM((n_tok, d_model), BF16),
                pltpu.VMEM((tok_dev, d_model), BF16),
                pltpu.VMEM((pairs, ffn), BF16),
                pltpu.VMEM((RING1 + EXTRA, 2, 2, KU, ffn), BF16),
                pltpu.VMEM((RING2, EPS, ffn, DB), BF16),
                pltpu.VMEM((3, tok_dev, d_model), BF16),
                pltpu.VMEM((pairs, DB), BF16),
                pltpu.VMEM((2, 2, 2 * CAP, KU), BF16),
                pltpu.VMEM((3, top_k, tok_dev), jnp.int32),
                pltpu.VMEM((3, top_k, tok_dev), F32),
                pltpu.VMEM((n_exp, n_tok), jnp.int32),
                pltpu.VMEM((n_tok, 8), F32),
                dma((RING1 + EXTRA, 2)),
                dma((RING2,)),
                dma((2,)),
                dma((2, 3)),
                dma((2, 3)),
                dma((3, len(BLOCKS))),
                dma((3, len(BLOCKS))),
                dma((3, d_model // DB)),
                dma((3, d_model // DB)),
                dma((d_model // DB,)),
            ],
            compiler_params=pltpu.CompilerParams(collective_id=0, has_side_effects=True, vmem_limit_bytes=67043328),
        )(tokens, expert_ids.T, gate_vals.T, w_gate.reshape(units), w_up.reshape(units), w_down)

    return jax.shard_map(device_step, mesh=mesh, in_specs=(row_spec, row_spec, row_spec, expert_spec, expert_spec, expert_spec), out_specs=row_spec, check_vma=False)
```

```python
import jax
import jax.numpy as jnp
from jax import lax
from jax.experimental import pallas as pl
from jax.experimental.pallas import tpu as pltpu
from jax.sharding import PartitionSpec as P

MESH = pl.DeviceIdType.MESH
F32, BF16 = jnp.float32, jnp.bfloat16
GROUPS = 4
CAP = 128
KU = 256
DB = 256
RING1 = 8
EXTRA = 4
PER_BODY = 2
EPS = 4
RING2 = 4


def layer_kernel(tok, ids_in, gts_in, w_gate, w_up, w_down, out, acc, rows_all, hid, ring1, ring2, back,
                 y_blk, xbuf, ids_all, gts_all, slots, tbl, w1_sem, w2_sem, loc_sem, idx_send, idx_recv, d_send, d_recv,
                 r_send, r_recv, o_sem):
    tok_dev, d_model = tok.shape
    n_exp, n_unit, _, ffn = w_gate.shape
    n_tok = GROUPS * tok_dev
    n_kb, n_db, n_grp = 2 + (n_unit - 2) // 2, d_model // DB, n_exp // EPS
    n_one, n_two = n_exp // 4, n_exp // 2
    steps2 = n_db * n_grp

    me = lax.axis_index('ep')
    sib = me + 1 - 2 * lax.rem(me, 2)
    over = lax.rem(me + 2, GROUPS)
    diag = lax.rem(sib + 2, GROUPS)
    peers = (over, diag, sib)

    def rows_of(dev):
        return pl.ds(pl.multiple_of(dev * tok_dev, tok_dev), tok_dev)

    def first_unit(k):
        return k if isinstance(k, int) and k < 2 else 2 * k - 2

    def w1_copies(k, i, slot):
        if isinstance(k, int) and k < 2:
            part = (pl.ds(i * 2, 2), k)
        else:
            part = (i, pl.ds(first_unit(k), 2))
        return (pltpu.make_async_copy(w_gate.at[part], ring1.at[slot, 0], w1_sem.at[slot, 0]),
                pltpu.make_async_copy(w_up.at[part], ring1.at[slot, 1], w1_sem.at[slot, 1]))

    def block_cols(k):
        if isinstance(k, int):
            return pl.ds(first_unit(k) * KU, KU if k < 2 else 2 * KU)
        return pl.ds(pl.multiple_of(first_unit(k) * KU, 2 * KU), 2 * KU)

    def w2_copy(step, slot):
        g, d = lax.rem(step, n_grp), lax.div(step, n_grp)
        cols = pl.ds(pl.multiple_of(d * DB, DB), DB)
        return pltpu.make_async_copy(w_down.at[pl.ds(g * EPS, EPS), :, cols], ring2.at[slot], w2_sem.at[slot])

    mine_copy = pltpu.make_async_copy(tok, rows_all.at[rows_of(me), :], loc_sem.at[0])
    mine_copy.start()
    barrier = pltpu.get_barrier_semaphore()
    for dev in peers:
        pl.semaphore_signal(barrier, inc=1, device_id={'ep': dev}, device_id_type=MESH)

    def start0(i, c):
        for copy in w1_copies(0, i, i):
            copy.start()
        return c

    lax.fori_loop(0, RING1, start0, 0)
    pl.semaphore_wait(barrier, len(peers))

    def idx_copy(j, what):
        src, dst = (ids_in, ids_all) if what == 0 else (gts_in, gts_all)
        return pltpu.make_async_remote_copy(src_ref=src, dst_ref=dst.at[j], send_sem=idx_send.at[what, j], recv_sem=idx_recv.at[what, j],
                                            device_id={'ep': peers[j]}, device_id_type=MESH)

    def disp_copy(kind, k):
        cols = block_cols(k)
        rows = rows_all.at[rows_of(over if kind == 2 else me), cols]
        return pltpu.make_async_remote_copy(src_ref=rows, dst_ref=rows, send_sem=d_send.at[kind, k], recv_sem=d_recv.at[kind, k],
                                            device_id={'ep': over if kind == 0 else sib}, device_id_type=MESH)

    def disp_arrival(kind, k):
        cols = block_cols(k)
        dst = rows_all.at[rows_of((over, sib, diag)[kind]), cols]
        return pltpu.make_async_remote_copy(src_ref=dst, dst_ref=dst, send_sem=d_send.at[kind, k], recv_sem=d_recv.at[kind, k],
                                            device_id={'ep': over if kind == 0 else sib}, device_id_type=MESH)

    for j in range(3):
        for what in range(2):
            idx_copy(j, what).start()
    mine_copy.wait()
    for k in range(n_kb):
        disp_copy(0, k).start()
        disp_copy(1, k).start()

    def start1(i, c):
        for copy in w1_copies(1, i, RING1 + i):
            copy.start()
        return c

    def start2(g, c):
        w2_copy(g, g).start()
        return c

    lax.fori_loop(0, EXTRA, start1, 0)
    lax.fori_loop(0, RING2, start2, 0)

    for j in range(3):
        for what in range(2):
            idx_copy(j, what).wait()

    expert = lax.broadcasted_iota(jnp.int32, (n_exp, tok_dev), 0) + me * n_exp

    def side(ids_ref, gts_ref):
        ids, gts = ids_ref[...], gts_ref[...]
        hit_any = jnp.zeros((n_exp, tok_dev), jnp.int32)
        gate = jnp.zeros((n_exp, tok_dev), F32)
        for j in range(ids.shape[0]):
            hit = ids[j:j + 1, :] == expert
            hit_any = hit_any + jnp.where(hit, 1, 0)
            gate = gate + jnp.where(hit, gts[j:j + 1, :], 0.0)
        return hit_any, gate

    parts = [side(ids_in, gts_in)] + [side(ids_all.at[j], gts_all.at[j]) for j in range(3)]

    def of_device(b, i):
        p = [part[i] for part in parts]
        return jnp.where(me == b, p[0], jnp.where(over == b, p[1], jnp.where(diag == b, p[2], p[3])))

    member = jnp.concatenate([of_device(b, 0) for b in range(GROUPS)], axis=1)
    gate = jnp.concatenate([of_device(b, 1) for b in range(GROUPS)], axis=1)
    lane = lax.broadcasted_iota(jnp.int32, (n_exp, n_tok), 1)
    count = member
    shift = 1
    while shift < n_tok:
        count = count + jnp.where(lane >= shift, pltpu.roll(count, shift, 1), 0)
        shift *= 2
    is_mem = member > 0
    slot = jnp.where(is_mem, count - 1, -1)
    slots[...] = slot
    pos = lax.broadcasted_iota(jnp.int32, (n_exp, n_tok), 0) * CAP + slot
    big = n_exp * CAP
    pos1 = jnp.min(jnp.where(is_mem, pos, big), axis=0, keepdims=True)
    pos2 = jnp.max(jnp.where(is_mem, pos, -1), axis=0, keepdims=True)
    g1 = jnp.sum(jnp.where(is_mem & (pos == pos1), gate, 0.0), axis=0, keepdims=True)
    g2 = jnp.sum(jnp.where(is_mem & (pos == pos2), gate, 0.0), axis=0, keepdims=True)
    sub = lax.broadcasted_iota(jnp.int32, (8, n_tok), 0)
    packed = jnp.where(sub == 0, pos1.astype(F32), jnp.where(sub == 1, pos2.astype(F32), jnp.where(sub == 2, g1, jnp.where(sub == 3, g2, 0.0))))
    tbl[...] = jnp.transpose(packed)

    def clear(i, c):
        acc[pl.ds(pl.multiple_of(i * CAP, CAP), CAP), :] = jnp.zeros((CAP, 2 * ffn), F32)
        return c

    lax.fori_loop(0, n_exp, clear, 0)

    half = big // 2
    pick_rows = n_tok // (n_two * (n_kb - 3))

    def build_picks(i):
        per = tok_dev // pick_rows
        dev, r = lax.div(i, per), pl.multiple_of(lax.rem(i, per) * pick_rows, pick_rows)
        t = tbl[pl.ds(pl.multiple_of(i * pick_rows, pick_rows), pick_rows), :]
        for h in range(2):
            at = (lax.broadcasted_iota(jnp.int32, (pick_rows, half), 1) + h * half).astype(F32)
            for p in range(2):
                ring1[RING1 + dev, h, p, pl.ds(r, pick_rows), :] = jnp.where(t[:, p:p + 1] == at, 1.0, 0.0).astype(BF16)

    def fan(cols, e, n, par):
        at = lax.broadcasted_iota(jnp.int32, (CAP, n_tok), 0)
        hot = jnp.concatenate([jnp.where(at == slots[pl.ds(e + m, 1), :], 1.0, 0.0).astype(BF16) for m in range(n)], axis=0)
        x = jnp.dot(hot, rows_all[:, cols], preferred_element_type=F32).astype(BF16)
        for u in range(2):
            xbuf[par, u] = x[:, u * KU:(u + 1) * KU] if n == 2 else x[u * 2 * CAP:(u + 1) * 2 * CAP, :]

    def down(e, ring, i):
        r = pl.ds(pl.multiple_of(e * CAP, CAP), CAP)
        y_blk[r, :] = jnp.dot(hid[r, :], ring2[ring, i], preferred_element_type=F32).astype(BF16)

    def ffn_in(e, n, rings, par, final, cw):
        for m in range(n):
            ring = rings[m // (n // PER_BODY)]
            r = pl.ds(pl.multiple_of((e + m) * CAP, CAP), CAP)
            for c0 in range(0, ffn, cw):
                acts = []
                for p in range(2):
                    cols = pl.ds(c0, cw)
                    if n == 2:
                        xr = pl.ds(m * CAP, CAP)
                        act = (jnp.dot(xbuf[par, 0, xr, :], ring1[ring, p, 0, :, cols], preferred_element_type=F32) +
                               jnp.dot(xbuf[par, 1, xr, :], ring1[ring, p, 1, :, cols], preferred_element_type=F32))
                    else:
                        act = jnp.dot(xbuf[par, m // 2, pl.ds((m % 2) * CAP, CAP), :], ring1[ring, p, m % 2, :, cols], preferred_element_type=F32)
                    acc_cols = pl.ds(p * ffn + c0, cw)
                    act = acc[r, acc_cols] + act
                    if not final:
                        acc[r, acc_cols] = act
                    acts.append(act)
                if final:
                    hid[r, cols] = (jax.nn.silu(acts[0]) * acts[1]).astype(BF16)

    def take(k):
        disp_arrival(1, k).wait_recv()
        disp_arrival(2, k).wait_recv()

    def hand_on(k):
        disp_arrival(0, k).wait_recv()
        disp_copy(2, k).start()

    def begin(i, slot0, n_slots, k):
        rings = [lax.rem(i * PER_BODY + m + slot0, n_slots) for m in range(PER_BODY)]
        for m in range(PER_BODY):
            for copy in w1_copies(k, 0, rings[m]):
                copy.wait()
        return rings

    def refill(k, i, slot):
        for copy in w1_copies(k, i, slot):
            copy.start()

    hand_on(0)
    take(0)
    fan(block_cols(0), 0, 4, 0)

    def loop_one(i, c):
        @pl.when(i == n_one - 1)
        def _():
            take(1)

        rings = begin(i, 0, RING1 + EXTRA, 0)
        par = lax.rem(i, 2)
        ffn_in(lax.rem(i, n_one) * 4, 4, rings, par, False, ffn)
        nxt = lax.rem(i + 1, 2 * n_one)
        fan(pl.ds(pl.multiple_of(lax.div(nxt, n_one) * KU, KU), KU), lax.rem(nxt, n_one) * 4, 4, 1 - par)

        @pl.when(i < 2)
        def _():
            for m in range(PER_BODY):
                refill(1, i * 2 + m + EXTRA, rings[m])

        @pl.when(i * (i - 4) * (i - 5) * (i - 1) > 0)
        def _():
            for m in range(PER_BODY):
                refill(2, i * 2 + m - 4 - 4 * lax.div(i, 6), rings[m])

        @pl.when(i == n_one - 3)
        def _():
            hand_on(1)

        @pl.when(i == 2 * n_one - 3)
        def _():
            hand_on(2)
        return c

    lax.fori_loop(0, 2 * n_one, loop_one, 0)
    take(2)
    fan(block_cols(2), 0, 2, 0)

    def loop_two(i, c):
        k = 2 + lax.div(i, n_two)

        @pl.when(lax.rem(i, n_two) == n_two - 1)
        def _():
            take(k + 1)

        rings = begin(i, RING1 - EXTRA, RING1, 2)
        par = lax.rem(i, 2)
        ffn_in(lax.rem(i, n_two) * 2, 2, rings, par, False, ffn)
        nxt = i + 1
        fan(block_cols(2 + lax.div(nxt, n_two)), lax.rem(nxt, n_two) * 2, 2, 1 - par)
        build_picks(i)
        for m in range(PER_BODY):
            ahead = i * 2 + m + RING1
            refill(2 + lax.div(ahead, n_exp), lax.rem(ahead, n_exp), rings[m])

        @pl.when(lax.rem(i, n_two) == n_two - 3)
        def _():
            hand_on(k + 1)
        return c

    lax.fori_loop(0, n_two * (n_kb - 3), loop_two, 0)
    for g in range(RING2):
        w2_copy(g, g).wait()

    def loop_last(i, c):
        rings = begin(i, RING1 - EXTRA, RING1, 2)
        par = lax.rem(i, 2)
        ffn_in(i * 2, 2, rings, par, True, DB)
        fan(block_cols(n_kb - 1), lax.rem(i + 1, n_two) * 2, 2, 1 - par)
        before = lax.rem(i + n_two - 1, n_two) * 2
        for m in range(2):
            down(before + m, lax.div(before, EPS), lax.rem(before, EPS) + m)

        @pl.when(i * 2 + RING1 < n_exp)
        def _():
            for m in range(PER_BODY):
                refill(n_kb - 1, i * 2 + m + RING1, rings[m])
        return c

    lax.fori_loop(0, n_two, loop_last, 0)
    for m in range(2):
        down(n_exp - 2 + m, n_grp - 1, EPS - 2 + m)

    def refill2(g, c):
        w2_copy(n_grp + g, g).start()
        return c

    lax.fori_loop(0, RING2, refill2, 0)

    for k in range(n_kb):
        for kind in range(3):
            disp_copy(kind, k).wait_send()

    def stage(slot, d):
        per = ffn // DB
        return (slot, 0, lax.div(d, per), slice(None), pl.ds(pl.multiple_of(lax.rem(d, per) * DB, DB), DB))

    def ret_copy(j, d):
        cols = pl.ds(pl.multiple_of(d * DB, DB), DB)
        return pltpu.make_async_remote_copy(src_ref=rows_all.at[rows_of(peers[j]), cols], dst_ref=back.at[j, :, cols],
                                            send_sem=r_send.at[j, d], recv_sem=r_recv.at[j, d], device_id={'ep': peers[j]}, device_id_type=MESH)

    def combine(d):
        cols = pl.ds(pl.multiple_of(d * DB, DB), DB)

        def one(j, c):
            dev = lax.rem(me + (sib - me) * lax.rem(lax.div(j + 1, 2), 2) + 2 - 2 * lax.div(j, 2), GROUPS)
            r = rows_of(dev)
            y1, y2 = (sum(jnp.dot(ring1[RING1 + dev, h, p], y_blk[h * half:(h + 1) * half, :], preferred_element_type=F32) for h in range(2)) for p in range(2))
            sums = (tbl[r, 2:3] * y1 + tbl[r, 3:4] * y2).astype(BF16)

            @pl.when(j < 3)
            def _():
                rows_all[r, cols] = sums
                pltpu.make_async_remote_copy(src_ref=rows_all.at[r, cols], dst_ref=back.at[j, :, cols], send_sem=r_send.at[j, d], recv_sem=r_recv.at[j, d],
                                             device_id={'ep': dev}, device_id_type=MESH).start()

            @pl.when(j == 3)
            def _():
                ring1[stage(0, d)] = sums
            return c

        lax.fori_loop(0, GROUPS, one, 0)

    def block2(d, c):
        def step2(g, c2):
            step = d * n_grp + g
            ring = lax.rem(step, RING2)
            w2_copy(step, ring).wait()
            for i in range(EPS):
                down(g * EPS + i, ring, i)

            @pl.when(step + RING2 < steps2)
            def _():
                w2_copy(step + RING2, ring).start()
            return c2

        @pl.when(d > 0)
        def _():
            lax.fori_loop(0, n_grp, step2, 0)

        combine(d)
        return c

    lax.fori_loop(0, n_db, block2, 0)

    def out_copy(d):
        cols = pl.ds(pl.multiple_of(d * DB, DB), DB)
        return pltpu.make_async_copy(ring1.at[stage(1, d)], out.at[:, cols], o_sem.at[d])

    def finish(d, c):
        cols = pl.ds(pl.multiple_of(d * DB, DB), DB)
        for j in range(3):
            ret_copy(j, d).wait_recv()
        total = rows_all[rows_of(me), cols].astype(F32) + ring1[stage(0, d)].astype(F32)
        for j in range(3):
            total = total + back[j, :, cols].astype(F32)
        ring1[stage(1, d)] = total.astype(BF16)
        out_copy(d).start()
        return c

    lax.fori_loop(0, n_db, finish, 0)

    def drain(d, c):
        for j in range(3):
            ret_copy(j, d).wait_send()
        out_copy(d).wait()
        return c

    lax.fori_loop(0, n_db, drain, 0)


def solution(mesh):
    row_spec = P(('dp', 'ep'))
    expert_spec = P('ep')

    def device_step(tokens, expert_ids, gate_vals, w_gate, w_up, w_down):
        tok_dev, d_model = tokens.shape
        n_exp, _, ffn = w_gate.shape
        top_k = expert_ids.shape[1]
        n_tok = GROUPS * tok_dev
        pairs = n_exp * CAP
        units = (n_exp, d_model // KU, KU, ffn)
        hbm = pl.BlockSpec(memory_space=pltpu.HBM)
        vmem = pl.BlockSpec(memory_space=pltpu.VMEM)
        dma = pltpu.SemaphoreType.DMA
        return pl.pallas_call(
            layer_kernel,
            out_shape=jax.ShapeDtypeStruct((tok_dev, d_model), BF16),
            in_specs=[hbm, vmem, vmem, hbm, hbm, hbm],
            out_specs=hbm,
            scratch_shapes=[
                pltpu.VMEM((pairs, 2 * ffn), F32),
                pltpu.VMEM((n_tok, d_model), BF16),
                pltpu.VMEM((pairs, ffn), BF16),
                pltpu.VMEM((RING1 + EXTRA, 2, 2, KU, ffn), BF16),
                pltpu.VMEM((RING2, EPS, ffn, DB), BF16),
                pltpu.VMEM((3, tok_dev, d_model), BF16),
                pltpu.VMEM((pairs, DB), BF16),
                pltpu.VMEM((2, 2, 2 * CAP, KU), BF16),
                pltpu.VMEM((3, top_k, tok_dev), jnp.int32),
                pltpu.VMEM((3, top_k, tok_dev), F32),
                pltpu.VMEM((n_exp, n_tok), jnp.int32),
                pltpu.VMEM((n_tok, 8), F32),
                dma((RING1 + EXTRA, 2)),
                dma((RING2,)),
                dma((1,)),
                dma((2, 3)),
                dma((2, 3)),
                dma((3, 2 + (d_model // KU - 2) // 2)),
                dma((3, 2 + (d_model // KU - 2) // 2)),
                dma((3, d_model // DB)),
                dma((3, d_model // DB)),
                dma((d_model // DB,)),
            ],
            compiler_params=pltpu.CompilerParams(collective_id=0, has_side_effects=True, vmem_limit_bytes=67043328),
        )(tokens, expert_ids.T, gate_vals.T, w_gate.reshape(units), w_up.reshape(units), w_down)

    return jax.shard_map(device_step, mesh=mesh, in_specs=(row_spec, row_spec, row_spec, expert_spec, expert_spec, expert_spec), out_specs=row_spec, check_vma=False)
```

```python
import functools

import jax
import jax.numpy as jnp
from jax import lax
from jax.experimental import pallas as pl
from jax.experimental.pallas import tpu as pltpu
from jax.sharding import PartitionSpec as P

MESH = pl.DeviceIdType.MESH
F32, BF16 = jnp.float32, jnp.bfloat16
GROUPS = 4
CAP = 128
KU = 256
DB = 256
RING1 = 8
EXTRA = 4
PER_BODY = 2
EPS = 4
RING2 = 4
FINAL_COLS = 512


def layer_kernel(tok, ids_hbm, gts_hbm, w_gate, w_up, w_down, out, acc, rows_all, hid, ring1, ring2, back,
                 y_blk, xbuf, ids_in, gts_in, ids_all, gts_all, slots, tbl, w1_sem, w2_sem, loc_sem, idx_send, idx_recv, d_send, d_recv,
                 r_send, r_recv, o_sem):
    tok_dev, d_model = tok.shape
    n_exp, n_unit, _, ffn = w_gate.shape
    n_tok = GROUPS * tok_dev
    n_kb, n_db, n_grp = 2 + (n_unit - 2) // 2, d_model // DB, n_exp // EPS
    n_one, n_two = n_exp // (2 * PER_BODY), n_exp // PER_BODY
    assert EPS % PER_BODY == 0 and n_exp == GROUPS * EPS and n_one * PER_BODY == RING1 == 2 * EXTRA
    steps2 = n_db * n_grp

    me = lax.axis_index('ep')
    sib = me + 1 - 2 * lax.rem(me, 2)
    over = lax.rem(me + 2, GROUPS)
    diag = lax.rem(sib + 2, GROUPS)
    peers = (over, diag, sib)

    def rows_of(dev):
        return pl.ds(pl.multiple_of(dev * tok_dev, tok_dev), tok_dev)

    def first_unit(k):
        return k if isinstance(k, int) and k < 2 else 2 * k - 2

    def pair_of(slot):
        return lax.div(slot, 2)

    def w1_copies(k, i, slot):
        if isinstance(k, int) and k < 2:
            part = (pl.ds(i * 2, 2), k)
        else:
            part = (i, pl.ds(first_unit(k), 2))
        return (pltpu.make_async_copy(w_gate.at[part], ring1.at[slot, 0], w1_sem.at[pair_of(slot)]),
                pltpu.make_async_copy(w_up.at[part], ring1.at[slot, 1], w1_sem.at[pair_of(slot)]))

    def block_cols(k):
        if isinstance(k, int):
            return pl.ds(first_unit(k) * KU, KU if k < 2 else 2 * KU)
        return pl.ds(pl.multiple_of(first_unit(k) * KU, 2 * KU), 2 * KU)

    def w2_copy(step, slot):
        g, d = lax.rem(step, n_grp), lax.div(step, n_grp)
        cols = pl.ds(pl.multiple_of(d * DB, DB), DB)
        return pltpu.make_async_copy(w_down.at[pl.ds(g * EPS, EPS), :, cols], ring2.at[slot], w2_sem.at[slot])

    mine_copy = pltpu.make_async_copy(tok, rows_all.at[rows_of(me), :], loc_sem.at[0])
    mine_copy.start()
    ids_copy = pltpu.make_async_copy(ids_hbm, ids_in, loc_sem.at[1])
    gts_copy = pltpu.make_async_copy(gts_hbm, gts_in, loc_sem.at[2])
    ids_copy.start()
    gts_copy.start()
    barrier = pltpu.get_barrier_semaphore()
    for dev in peers:
        pl.semaphore_signal(barrier, inc=1, device_id={'ep': dev}, device_id_type=MESH)

    def start0(i, c):
        for copy in w1_copies(0, i, i):
            copy.start()
        return c

    lax.fori_loop(0, RING1, start0, 0)
    pl.semaphore_wait(barrier, len(peers))

    def idx_copy(j, what):
        src, dst = (ids_in, ids_all) if what == 0 else (gts_in, gts_all)
        return pltpu.make_async_remote_copy(src_ref=src, dst_ref=dst.at[j], send_sem=idx_send.at[what, j], recv_sem=idx_recv.at[what, j],
                                            device_id={'ep': peers[j]}, device_id_type=MESH)

    def disp_copy(kind, k):
        cols = block_cols(k)
        rows = rows_all.at[rows_of(over if kind == 2 else me), cols]
        return pltpu.make_async_remote_copy(src_ref=rows, dst_ref=rows, send_sem=d_send.at[kind, k], recv_sem=d_recv.at[kind, k],
                                            device_id={'ep': over if kind == 0 else sib}, device_id_type=MESH)

    def disp_arrival(kind, k):
        cols = block_cols(k)
        dst = rows_all.at[rows_of((over, sib, diag)[kind]), cols]
        return pltpu.make_async_remote_copy(src_ref=dst, dst_ref=dst, send_sem=d_send.at[kind, k], recv_sem=d_recv.at[kind, k],
                                            device_id={'ep': over if kind == 0 else sib}, device_id_type=MESH)

    mine_copy.wait()
    disp_copy(0, 0).start()
    disp_copy(1, 0).start()
    ids_copy.wait()
    gts_copy.wait()
    for j in range(3):
        for what in range(2):
            idx_copy(j, what).start()
    for k in range(1, n_kb):
        disp_copy(0, k).start()
        disp_copy(1, k).start()

    def start1(i, c):
        for copy in w1_copies(1, i, RING1 + i):
            copy.start()
        return c

    def start2(g, c):
        w2_copy(g, g).start()
        return c

    lax.fori_loop(0, EXTRA, start1, 0)
    lax.fori_loop(0, RING2, start2, 0)

    for j in range(3):
        for what in range(2):
            idx_copy(j, what).wait()

    expert = lax.broadcasted_iota(jnp.int32, (n_exp, tok_dev), 0) + me * n_exp

    def side(ids_ref, gts_ref):
        ids, gts = ids_ref[...], gts_ref[...]
        hit_any = jnp.zeros((n_exp, tok_dev), jnp.int32)
        gate = jnp.zeros((n_exp, tok_dev), F32)
        for j in range(ids.shape[0]):
            hit = ids[j:j + 1, :] == expert
            hit_any = hit_any + jnp.where(hit, 1, 0)
            gate = gate + jnp.where(hit, gts[j:j + 1, :], 0.0)
        return hit_any, gate

    parts = [side(ids_in, gts_in)] + [side(ids_all.at[j], gts_all.at[j]) for j in range(3)]

    def of_device(b, i):
        p = [part[i] for part in parts]
        return jnp.where(me == b, p[0], jnp.where(over == b, p[1], jnp.where(diag == b, p[2], p[3])))

    member = jnp.concatenate([of_device(b, 0) for b in range(GROUPS)], axis=1)
    gate = jnp.concatenate([of_device(b, 1) for b in range(GROUPS)], axis=1)
    lane = lax.broadcasted_iota(jnp.int32, (n_exp, n_tok), 1)
    count = member
    shift = 1
    while shift < n_tok:
        count = count + jnp.where(lane >= shift, pltpu.roll(count, shift, 1), 0)
        shift *= 2
    is_mem = member > 0
    slot = jnp.where(is_mem, count - 1, -1)
    slots[...] = slot
    pos = lax.broadcasted_iota(jnp.int32, (n_exp, n_tok), 0) * CAP + slot
    big = n_exp * CAP
    pos1 = jnp.min(jnp.where(is_mem, pos, big), axis=0, keepdims=True)
    pos2 = jnp.max(jnp.where(is_mem, pos, -1), axis=0, keepdims=True)
    g1 = jnp.sum(jnp.where(is_mem & (pos == pos1), gate, 0.0), axis=0, keepdims=True)
    g2 = jnp.sum(jnp.where(is_mem & (pos == pos2), gate, 0.0), axis=0, keepdims=True)
    sub = lax.broadcasted_iota(jnp.int32, (8, n_tok), 0)
    packed = jnp.where(sub == 0, pos1.astype(F32), jnp.where(sub == 1, pos2.astype(F32), jnp.where(sub == 2, g1, jnp.where(sub == 3, g2, 0.0))))
    tbl[...] = packed

    half = big // 2

    def build_picks(i):
        b, h = (i // 2, i % 2) if isinstance(i, int) else (lax.div(i, 2), lax.rem(i, 2))
        per = tok_dev // CAP
        dev, r = (b // per, b % per * CAP) if isinstance(i, int) else (lax.div(b, per), pl.multiple_of(lax.rem(b, per) * CAP, CAP))
        t = jnp.transpose(tbl[:, pl.ds(b * CAP if isinstance(i, int) else pl.multiple_of(b * CAP, CAP), CAP)])
        at = (lax.broadcasted_iota(jnp.int32, (CAP, half), 1) + h * half).astype(F32)
        for p in range(2):
            ring1[RING1 + dev, h, p, pl.ds(r, CAP), :] = jnp.where(t[:, p:p + 1] == at, 1.0, 0.0).astype(BF16)

    def fan(cols, e, n, par):
        at = lax.broadcasted_iota(jnp.int32, (CAP, n_tok), 0)
        for q in range(n // 2):
            hot = jnp.concatenate([jnp.where(at == slots[pl.ds(e + 2 * q + m, 1), :], 1.0, 0.0).astype(BF16) for m in range(2)], axis=0)
            x = jnp.dot(hot, rows_all[:, cols], preferred_element_type=F32).astype(BF16)
            for u in range(x.shape[1] // KU):
                xbuf[par, u, q] = x[:, u * KU:(u + 1) * KU]

    def down(e, ring, i):
        r = pl.ds(pl.multiple_of(e * CAP, CAP), CAP)
        y_blk[r, :] = jnp.dot(hid[r, :], ring2[ring, i], preferred_element_type=F32).astype(BF16)

    def ffn_in(e, rings, par, two, first, final, cw):
        for m in range(len(rings) * (1 if two else 2)):
            ring, xr = rings[m if two else m // 2], pl.ds((m % 2) * CAP, CAP)
            r = pl.ds(pl.multiple_of((e + m) * CAP, CAP), CAP)
            for c0 in range(0, ffn, cw):
                acts = []
                for p in range(2):
                    cols = pl.ds(c0, cw)
                    if two:
                        act = (jnp.dot(xbuf[par, 0, m // 2, xr, :], ring1[ring, p, 0, :, cols], preferred_element_type=F32) +
                               jnp.dot(xbuf[par, 1, m // 2, xr, :], ring1[ring, p, 1, :, cols], preferred_element_type=F32))
                    else:
                        act = jnp.dot(xbuf[par, 0, m // 2, xr, :], ring1[ring, p, m % 2, :, cols], preferred_element_type=F32)
                    acc_cols = pl.ds(p * ffn + c0, cw)
                    if not first:
                        act = acc[r, acc_cols] + act
                    if not final:
                        acc[r, acc_cols] = act
                    acts.append(act)
                if final:
                    hid[r, cols] = (jax.nn.silu(acts[0]) * acts[1]).astype(BF16)

    def take(k):
        disp_arrival(1, k).wait_recv()
        disp_arrival(2, k).wait_recv()

    def hand_on(k):
        disp_arrival(0, k).wait_recv()
        disp_copy(2, k).start()

    def begin(k, i):
        rem = (lambda a, b: a % b) if isinstance(i, int) else lax.rem
        slot = i * PER_BODY if k == 0 else rem(i * PER_BODY + RING1, RING1 + EXTRA) if k == 1 else rem(i * PER_BODY + RING1 - EXTRA, RING1)
        both = ring1.at[pl.ds(slot, PER_BODY)]
        pltpu.make_async_copy(both, both, w1_sem.at[pair_of(slot)]).wait()
        return [slot + m for m in range(PER_BODY)]

    def refill(k, i, slot):
        for copy in w1_copies(k, i, slot):
            copy.start()

    def body(k, i, nxt, before=None):
        static = isinstance(i, int)
        two, final = k >= 2, k == n_kb - 1
        per, n_body = (PER_BODY, n_two) if two else (2 * PER_BODY, n_one)
        par = i % 2 if static else lax.rem(i, 2)
        rings = begin(k, i)
        ffn_in(i * per, rings, par, two, k == 0, final, FINAL_COLS if final else ffn)
        if nxt is not None:
            fan(block_cols(nxt[0]), nxt[1] * (PER_BODY if nxt[0] >= 2 else 2 * PER_BODY), PER_BODY if nxt[0] >= 2 else 2 * PER_BODY, 1 - par)
        if before is not None:
            for m in range(PER_BODY):
                e = before * PER_BODY + m
                down(e, lax.div(e, EPS), lax.rem(e, EPS))
        if 2 <= k < 4:
            build_picks((k - 2) * n_body + i)

        def fill(kk, i0):
            for m in range(PER_BODY):
                refill(kk, i0 + m, rings[m])

        here, s0 = n_body * PER_BODY, i * PER_BODY
        when = (lambda c: (lambda f: f() if c else None)) if static else pl.when
        if k == 0:
            when(i < 2)(lambda: fill(1, s0 + EXTRA))
            when(i >= 2)(lambda: fill(2, s0 - EXTRA))
        elif k == 1:
            when(i >= 2)(lambda: fill(2, s0))
        elif final:
            when(s0 + RING1 < here)(lambda: fill(k, s0 + RING1))
        elif static:
            fill(k + (s0 + RING1) // here, (s0 + RING1) % here)
        else:
            fill(k + lax.div(s0 + RING1, here), lax.rem(s0 + RING1, here))

    hand_on(0)
    take(0)
    fan(block_cols(0), 0, 2 * PER_BODY, 0)
    for k in range(n_kb):
        n_body, final = n_two if k >= 2 else n_one, k == n_kb - 1
        if final:
            for g in range(RING2):
                w2_copy(g, g).wait()

        def loop(i, c, k=k, n_body=n_body, final=final):
            body(k, i, (k, i + 1), lax.rem(i + n_body - 1, n_body) if final else None)
            if not final:
                pl.when(i == n_body - 3)(functools.partial(hand_on, k + 1))
            return c

        lax.fori_loop(0, n_body - 1, loop, 0)
        if not final:
            take(k + 1)
        body(k, n_body - 1, None if final else (k + 1, 0), n_body - 2 if final else None)

    for m in range(EPS - PER_BODY, EPS):
        down(n_exp - EPS + m, n_grp - 1, m)

    def refill2(g, c):
        w2_copy(n_grp + g, g).start()
        return c

    lax.fori_loop(0, RING2, refill2, 0)

    for k in range(n_kb):
        for kind in range(3):
            disp_copy(kind, k).wait_send()

    def stage(slot, d):
        per = ffn // DB
        return (slot, 0, lax.div(d, per), slice(None), pl.ds(pl.multiple_of(lax.rem(d, per) * DB, DB), DB))

    def ret_copy(j, d):
        cols = pl.ds(pl.multiple_of(d * DB, DB), DB)
        return pltpu.make_async_remote_copy(src_ref=rows_all.at[rows_of(peers[j]), cols], dst_ref=back.at[j, :, cols],
                                            send_sem=r_send.at[j, d], recv_sem=r_recv.at[j, d], device_id={'ep': peers[j]}, device_id_type=MESH)

    def combine(d):
        cols = pl.ds(pl.multiple_of(d * DB, DB), DB)

        def one(j, c):
            dev = lax.rem(me + (sib - me) * lax.rem(lax.div(j + 1, 2), 2) + 2 - 2 * lax.div(j, 2), GROUPS)
            r = rows_of(dev)
            y1, y2 = (sum(jnp.dot(ring1[RING1 + dev, h, p], y_blk[h * half:(h + 1) * half, :], preferred_element_type=F32) for h in range(2)) for p in range(2))
            t = jnp.transpose(tbl[:, r])
            sums = (t[:, 2:3] * y1 + t[:, 3:4] * y2).astype(BF16)

            @pl.when(j < 3)
            def _():
                rows_all[r, cols] = sums
                pltpu.make_async_remote_copy(src_ref=rows_all.at[r, cols], dst_ref=back.at[j, :, cols], send_sem=r_send.at[j, d], recv_sem=r_recv.at[j, d],
                                             device_id={'ep': dev}, device_id_type=MESH).start()

            @pl.when(j == 3)
            def _():
                ring1[stage(0, d)] = sums
            return c

        lax.fori_loop(0, GROUPS, one, 0)

    def block2(d, c):
        def step2(g, c2):
            step = d * n_grp + g
            ring = lax.rem(step, RING2)
            w2_copy(step, ring).wait()
            for i in range(EPS):
                down(g * EPS + i, ring, i)

            @pl.when(step + RING2 < steps2)
            def _():
                w2_copy(step + RING2, ring).start()
            return c2

        @pl.when(d > 0)
        def _():
            lax.fori_loop(0, n_grp, step2, 0)

        combine(d)
        return c

    lax.fori_loop(0, n_db, block2, 0)

    def out_copy(d):
        cols = pl.ds(pl.multiple_of(d * DB, DB), DB)
        return pltpu.make_async_copy(ring1.at[stage(1, d)], out.at[:, cols], o_sem.at[d])

    def finish(d, c):
        cols = pl.ds(pl.multiple_of(d * DB, DB), DB)
        for j in range(3):
            ret_copy(j, d).wait_recv()
        total = rows_all[rows_of(me), cols].astype(F32) + ring1[stage(0, d)].astype(F32)
        for j in range(3):
            total = total + back[j, :, cols].astype(F32)
        ring1[stage(1, d)] = total.astype(BF16)
        out_copy(d).start()
        return c

    lax.fori_loop(0, n_db, finish, 0)

    def drain(d, c):
        for j in range(3):
            ret_copy(j, d).wait_send()
        out_copy(d).wait()
        return c

    lax.fori_loop(0, n_db, drain, 0)


def solution(mesh):
    row_spec = P(('dp', 'ep'))
    expert_spec = P('ep')

    def device_step(tokens, expert_ids, gate_vals, w_gate, w_up, w_down):
        tok_dev, d_model = tokens.shape
        n_exp, _, ffn = w_gate.shape
        top_k = expert_ids.shape[1]
        n_tok = GROUPS * tok_dev
        pairs = n_exp * CAP
        units = (n_exp, d_model // KU, KU, ffn)
        hbm = pl.BlockSpec(memory_space=pltpu.HBM)
        dma = pltpu.SemaphoreType.DMA
        return pl.pallas_call(
            layer_kernel,
            out_shape=jax.ShapeDtypeStruct((tok_dev, d_model), BF16),
            in_specs=[hbm] * 6,
            out_specs=hbm,
            scratch_shapes=[
                pltpu.VMEM((pairs, 2 * ffn), F32),
                pltpu.VMEM((n_tok, d_model), BF16),
                pltpu.VMEM((pairs, ffn), BF16),
                pltpu.VMEM((RING1 + EXTRA, 2, 2, KU, ffn), BF16),
                pltpu.VMEM((RING2, EPS, ffn, DB), BF16),
                pltpu.VMEM((3, tok_dev, d_model), BF16),
                pltpu.VMEM((pairs, DB), BF16),
                pltpu.VMEM((2, 2, 2, 2 * CAP, KU), BF16),
                pltpu.VMEM((top_k, tok_dev), jnp.int32),
                pltpu.VMEM((top_k, tok_dev), F32),
                pltpu.VMEM((3, top_k, tok_dev), jnp.int32),
                pltpu.VMEM((3, top_k, tok_dev), F32),
                pltpu.VMEM((n_exp, n_tok), jnp.int32),
                pltpu.VMEM((8, n_tok), F32),
                dma(((RING1 + EXTRA) // 2,)),
                dma((RING2,)),
                dma((3,)),
                dma((2, 3)),
                dma((2, 3)),
                dma((3, 2 + (d_model // KU - 2) // 2)),
                dma((3, 2 + (d_model // KU - 2) // 2)),
                dma((3, d_model // DB)),
                dma((3, d_model // DB)),
                dma((d_model // DB,)),
            ],
            compiler_params=pltpu.CompilerParams(collective_id=0, has_side_effects=True, vmem_limit_bytes=67043328),
        )(tokens, expert_ids.T, gate_vals.T, w_gate.reshape(units), w_up.reshape(units), w_down)

    return jax.shard_map(device_step, mesh=mesh, in_specs=(row_spec, row_spec, row_spec, expert_spec, expert_spec, expert_spec), out_specs=row_spec, check_vma=False)
```

```python
import functools

import jax
import jax.numpy as jnp
from jax import lax
from jax.experimental import pallas as pl
from jax.experimental.pallas import tpu as pltpu
from jax.sharding import PartitionSpec as P

MESH = pl.DeviceIdType.MESH
F32, BF16 = jnp.float32, jnp.bfloat16
GROUPS = 4
CAP = 128
KU = 256
DB = 256
RING1 = 8
EXTRA = 4
PER_BODY = 2
EPS = 4
RING2 = 4
FINAL_COLS = 512


def layer_kernel(tok, ids_hbm, gts_hbm, w_gate, w_up, w_down, out, acc, rows_all, hid, ring1, ring2, back,
                 y_blk, xbuf, ids_in, gts_in, ids_all, gts_all, slots, tbl, w1_sem, w2_sem, loc_sem, idx_send, idx_recv, d_send, d_recv,
                 r_send, r_recv):
    tok_dev, d_model = tok.shape
    n_exp, n_unit, _, ffn = w_gate.shape
    n_tok = GROUPS * tok_dev
    n_kb, n_db, n_grp = 2 + (n_unit - 2) // 2, d_model // DB, n_exp // EPS
    n_one, n_two = n_exp // (2 * PER_BODY), n_exp // PER_BODY
    assert EPS % PER_BODY == 0 and n_exp == GROUPS * EPS and n_one * PER_BODY == RING1 == 2 * EXTRA
    steps2 = n_db * n_grp

    me = lax.axis_index('ep')
    sib = me + 1 - 2 * lax.rem(me, 2)
    over = lax.rem(me + 2, GROUPS)
    diag = lax.rem(sib + 2, GROUPS)
    peers = (over, diag, sib)

    def rows_of(dev):
        return pl.ds(pl.multiple_of(dev * tok_dev, tok_dev), tok_dev)

    def first_unit(k):
        return k if isinstance(k, int) and k < 2 else 2 * k - 2

    def pair_of(slot):
        return lax.div(slot, 2)

    def w1_copies(k, i, slot):
        if isinstance(k, int) and k < 2:
            part = (pl.ds(i * 2, 2), k)
        else:
            part = (i, pl.ds(first_unit(k), 2))
        return (pltpu.make_async_copy(w_gate.at[part], ring1.at[slot, 0], w1_sem.at[pair_of(slot)]),
                pltpu.make_async_copy(w_up.at[part], ring1.at[slot, 1], w1_sem.at[pair_of(slot)]))

    def block_cols(k):
        if isinstance(k, int):
            return pl.ds(first_unit(k) * KU, KU if k < 2 else 2 * KU)
        return pl.ds(pl.multiple_of(first_unit(k) * KU, 2 * KU), 2 * KU)

    def w2_copy(step, slot):
        g, d = lax.rem(step, n_grp), lax.div(step, n_grp)
        cols = pl.ds(pl.multiple_of(d * DB, DB), DB)
        return pltpu.make_async_copy(w_down.at[pl.ds(g * EPS, EPS), :, cols], ring2.at[slot], w2_sem.at[slot])

    mine_copy = pltpu.make_async_copy(tok, rows_all.at[rows_of(me), :], loc_sem.at[0])
    ids_copy = pltpu.make_async_copy(ids_hbm, ids_in, loc_sem.at[1])
    gts_copy = pltpu.make_async_copy(gts_hbm, gts_in, loc_sem.at[2])
    ids_copy.start()
    gts_copy.start()
    mine_copy.start()
    barrier = pltpu.get_barrier_semaphore()
    for dev in peers:
        pl.semaphore_signal(barrier, inc=1, device_id={'ep': dev}, device_id_type=MESH)

    def start0(i, c):
        for copy in w1_copies(0, i, i):
            copy.start()
        return c

    lax.fori_loop(0, RING1, start0, 0)
    pl.semaphore_wait(barrier, len(peers))

    def idx_copy(j, what):
        src, dst = (ids_in, ids_all) if what == 0 else (gts_in, gts_all)
        return pltpu.make_async_remote_copy(src_ref=src, dst_ref=dst.at[j], send_sem=idx_send.at[what, j], recv_sem=idx_recv.at[what, j],
                                            device_id={'ep': peers[j]}, device_id_type=MESH)

    def disp_copy(kind, k):
        cols = block_cols(k)
        rows = rows_all.at[rows_of(over if kind == 2 else me), cols]
        return pltpu.make_async_remote_copy(src_ref=rows, dst_ref=rows, send_sem=d_send.at[kind, k], recv_sem=d_recv.at[kind, k],
                                            device_id={'ep': over if kind == 0 else sib}, device_id_type=MESH)

    def disp_arrival(kind, k):
        cols = block_cols(k)
        dst = rows_all.at[rows_of((over, sib, diag)[kind]), cols]
        return pltpu.make_async_remote_copy(src_ref=dst, dst_ref=dst, send_sem=d_send.at[kind, k], recv_sem=d_recv.at[kind, k],
                                            device_id={'ep': over if kind == 0 else sib}, device_id_type=MESH)

    ids_copy.wait()
    gts_copy.wait()
    for j in range(3):
        for what in range(2):
            idx_copy(j, what).start()
    mine_copy.wait()
    for k in range(n_kb):
        disp_copy(0, k).start()
        disp_copy(1, k).start()

    def start1(i, c):
        for copy in w1_copies(1, i, RING1 + i):
            copy.start()
        return c

    def start2(g, c):
        w2_copy(g, g).start()
        return c

    lax.fori_loop(0, EXTRA, start1, 0)
    lax.fori_loop(0, RING2, start2, 0)

    for j in range(3):
        for what in range(2):
            idx_copy(j, what).wait()

    expert = lax.broadcasted_iota(jnp.int32, (n_exp, tok_dev), 0) + me * n_exp

    def side(ids_ref, gts_ref):
        ids, gts = ids_ref[...], gts_ref[...]
        hit_any = jnp.zeros((n_exp, tok_dev), jnp.int32)
        gate = jnp.zeros((n_exp, tok_dev), F32)
        for j in range(ids.shape[0]):
            hit = ids[j:j + 1, :] == expert
            hit_any = hit_any + jnp.where(hit, 1, 0)
            gate = gate + jnp.where(hit, gts[j:j + 1, :], 0.0)
        return hit_any, gate

    parts = [side(ids_in, gts_in)] + [side(ids_all.at[j], gts_all.at[j]) for j in range(3)]

    def of_device(b, i):
        p = [part[i] for part in parts]
        return jnp.where(me == b, p[0], jnp.where(over == b, p[1], jnp.where(diag == b, p[2], p[3])))

    member = jnp.concatenate([of_device(b, 0) for b in range(GROUPS)], axis=1)
    gate = jnp.concatenate([of_device(b, 1) for b in range(GROUPS)], axis=1)
    lane = lax.broadcasted_iota(jnp.int32, (n_exp, n_tok), 1)
    count = member
    shift = 1
    while shift < n_tok:
        count = count + jnp.where(lane >= shift, pltpu.roll(count, shift, 1), 0)
        shift *= 2
    is_mem = member > 0
    slot = jnp.where(is_mem, count - 1, -1)
    slots[...] = slot
    pos = lax.broadcasted_iota(jnp.int32, (n_exp, n_tok), 0) * CAP + slot
    big = n_exp * CAP
    pos1 = jnp.min(jnp.where(is_mem, pos, big), axis=0, keepdims=True)
    pos2 = jnp.max(jnp.where(is_mem, pos, -1), axis=0, keepdims=True)
    g1 = jnp.sum(jnp.where(is_mem & (pos == pos1), gate, 0.0), axis=0, keepdims=True)
    g2 = jnp.sum(jnp.where(is_mem & (pos == pos2), gate, 0.0), axis=0, keepdims=True)
    sub = lax.broadcasted_iota(jnp.int32, (8, n_tok), 0)
    packed = jnp.where(sub == 0, pos1.astype(F32), jnp.where(sub == 1, pos2.astype(F32), jnp.where(sub == 2, g1, jnp.where(sub == 3, g2, 0.0))))
    tbl[...] = packed

    half = big // 2

    def build_picks(i):
        b, h = (i // 2, i % 2) if isinstance(i, int) else (lax.div(i, 2), lax.rem(i, 2))
        per = tok_dev // CAP
        dev, r = (b // per, b % per * CAP) if isinstance(i, int) else (lax.div(b, per), pl.multiple_of(lax.rem(b, per) * CAP, CAP))
        t = jnp.transpose(tbl[:, pl.ds(b * CAP if isinstance(i, int) else pl.multiple_of(b * CAP, CAP), CAP)])
        at = (lax.broadcasted_iota(jnp.int32, (CAP, half), 1) + h * half).astype(F32)
        for p in range(2):
            ring1[RING1 + dev, h, p, pl.ds(r, CAP), :] = jnp.where(t[:, p:p + 1] == at, 1.0, 0.0).astype(BF16)

    def fan(cols, e, n, par):
        at = lax.broadcasted_iota(jnp.int32, (CAP, n_tok), 0)
        for q in range(n // 2):
            hot = jnp.concatenate([jnp.where(at == slots[pl.ds(e + 2 * q + m, 1), :], 1.0, 0.0).astype(BF16) for m in range(2)], axis=0)
            x = jnp.dot(hot, rows_all[:, cols], preferred_element_type=F32).astype(BF16)
            for u in range(x.shape[1] // KU):
                xbuf[par, q + u] = x[:, u * KU:(u + 1) * KU]

    def down(e, ring, i):
        r = pl.ds(pl.multiple_of(e * CAP, CAP), CAP)
        y_blk[r, :] = jnp.dot(hid[r, :], ring2[ring, i], preferred_element_type=F32).astype(BF16)

    def ffn_in(e, rings, par, two, first, final, cw):
        for m in range(len(rings) * (1 if two else 2)):
            ring, xr = rings[m if two else m // 2], pl.ds((m % 2) * CAP, CAP)
            r = pl.ds(pl.multiple_of((e + m) * CAP, CAP), CAP)
            for c0 in range(0, ffn, cw):
                acts = []
                for p in range(2):
                    cols = pl.ds(c0, cw)
                    if two:
                        act = (jnp.dot(xbuf[par, 0, xr, :], ring1[ring, p, 0, :, cols], preferred_element_type=F32) +
                               jnp.dot(xbuf[par, 1, xr, :], ring1[ring, p, 1, :, cols], preferred_element_type=F32))
                    else:
                        act = jnp.dot(xbuf[par, m // 2, xr, :], ring1[ring, p, m % 2, :, cols], preferred_element_type=F32)
                    acc_cols = pl.ds(p * ffn + c0, cw)
                    if not first:
                        act = acc[r, acc_cols] + act
                    if not final:
                        acc[r, acc_cols] = act
                    acts.append(act)
                if final:
                    hid[r, cols] = (jax.nn.silu(acts[0]) * acts[1]).astype(BF16)

    def take(k):
        disp_arrival(1, k).wait_recv()
        disp_arrival(2, k).wait_recv()

    def hand_on(k):
        disp_arrival(0, k).wait_recv()
        disp_copy(2, k).start()

    def begin(k, i):
        rem = (lambda a, b: a % b) if isinstance(i, int) else lax.rem
        slot = i * PER_BODY if k == 0 else rem(i * PER_BODY + RING1, RING1 + EXTRA) if k == 1 else rem(i * PER_BODY + RING1 - EXTRA, RING1)
        both = ring1.at[pl.ds(slot, PER_BODY)]
        pltpu.make_async_copy(both, both, w1_sem.at[pair_of(slot)]).wait()
        return [slot + m for m in range(PER_BODY)]

    def refill(k, i, slot):
        for copy in w1_copies(k, i, slot):
            copy.start()

    def body(k, i, nxt, before=None):
        static = isinstance(i, int)
        two, final = k >= 2, k == n_kb - 1
        per, n_body = (PER_BODY, n_two) if two else (2 * PER_BODY, n_one)
        par = i % 2 if static else lax.rem(i, 2)
        rings = begin(k, i)
        ffn_in(i * per, rings, par, two, k == 0, final, FINAL_COLS if final else ffn)
        if nxt is not None:
            fan(block_cols(nxt[0]), nxt[1] * (PER_BODY if nxt[0] >= 2 else 2 * PER_BODY), PER_BODY if nxt[0] >= 2 else 2 * PER_BODY, 1 - par)
        if before is not None:
            for m in range(PER_BODY):
                e = before * PER_BODY + m
                down(e, lax.div(e, EPS), lax.rem(e, EPS))
        if 2 <= k < 4:
            build_picks((k - 2) * n_body + i)

        def fill(kk, i0):
            for m in range(PER_BODY):
                refill(kk, i0 + m, rings[m])

        here, s0 = n_body * PER_BODY, i * PER_BODY
        when = (lambda c: (lambda f: f() if c else None)) if static else pl.when
        if k == 0:
            when(i < 2)(lambda: fill(1, s0 + EXTRA))
            when(i >= 2)(lambda: fill(2, s0 - EXTRA))
        elif k == 1:
            when(i >= 2)(lambda: fill(2, s0))
        elif final:
            when(s0 + RING1 < here)(lambda: fill(k, s0 + RING1))
        elif static:
            fill(k + (s0 + RING1) // here, (s0 + RING1) % here)
        else:
            fill(k + lax.div(s0 + RING1, here), lax.rem(s0 + RING1, here))

    hand_on(0)
    take(0)
    fan(block_cols(0), 0, 2 * PER_BODY, 0)
    for k in range(n_kb):
        n_body, final = n_two if k >= 2 else n_one, k == n_kb - 1
        if final:
            for g in range(RING2):
                w2_copy(g, g).wait()

        def loop(i, c, k=k, n_body=n_body, final=final):
            body(k, i, (k, i + 1), lax.rem(i + n_body - 1, n_body) if final else None)
            if not final:
                pl.when(i == n_body - 3)(functools.partial(hand_on, k + 1))
            return c

        lax.fori_loop(0, n_body - 1, loop, 0)
        if not final:
            take(k + 1)
        body(k, n_body - 1, None if final else (k + 1, 0), n_body - 2 if final else None)

    for m in range(EPS - PER_BODY, EPS):
        down(n_exp - EPS + m, n_grp - 1, m)

    def refill2(g, c):
        w2_copy(n_grp + g, g).start()
        return c

    lax.fori_loop(0, RING2, refill2, 0)

    for k in range(n_kb):
        for kind in range(3):
            disp_copy(kind, k).wait_send()

    def stage(slot, d):
        per = ffn // DB
        return (slot, 0, lax.div(d, per), slice(None), pl.ds(pl.multiple_of(lax.rem(d, per) * DB, DB), DB))

    def ret_copy(j, d):
        cols = pl.ds(pl.multiple_of(d * DB, DB), DB)
        return pltpu.make_async_remote_copy(src_ref=rows_all.at[rows_of(peers[j]), cols], dst_ref=back.at[j, :, cols],
                                            send_sem=r_send.at[j, d], recv_sem=r_recv.at[j, d], device_id={'ep': peers[j]}, device_id_type=MESH)

    def combine(d):
        cols = pl.ds(pl.multiple_of(d * DB, DB), DB)

        def one(j, c):
            dev = lax.rem(me + (sib - me) * lax.rem(lax.div(j + 1, 2), 2) + 2 - 2 * lax.div(j, 2), GROUPS)
            r = rows_of(dev)
            y1, y2 = (sum(jnp.dot(ring1[RING1 + dev, h, p], y_blk[h * half:(h + 1) * half, :], preferred_element_type=F32) for h in range(2)) for p in range(2))
            t = jnp.transpose(tbl[:, r])
            sums = (t[:, 2:3] * y1 + t[:, 3:4] * y2).astype(BF16)

            @pl.when(j < 3)
            def _():
                rows_all[r, cols] = sums
                pltpu.make_async_remote_copy(src_ref=rows_all.at[r, cols], dst_ref=back.at[j, :, cols], send_sem=r_send.at[j, d], recv_sem=r_recv.at[j, d],
                                             device_id={'ep': dev}, device_id_type=MESH).start()

            @pl.when(j == 3)
            def _():
                ring1[stage(0, d)] = sums
            return c

        lax.fori_loop(0, GROUPS, one, 0)

    def block2(d, c):
        def step2(g, c2):
            step = d * n_grp + g
            ring = lax.rem(step, RING2)
            w2_copy(step, ring).wait()
            for i in range(EPS):
                down(g * EPS + i, ring, i)

            @pl.when(step + RING2 < steps2)
            def _():
                w2_copy(step + RING2, ring).start()
            return c2

        @pl.when(d > 0)
        def _():
            lax.fori_loop(0, n_grp, step2, 0)

        combine(d)
        return c

    lax.fori_loop(0, n_db, block2, 0)

    def finish(d, c):
        cols = pl.ds(pl.multiple_of(d * DB, DB), DB)
        for j in range(3):
            ret_copy(j, d).wait_recv()
        total = rows_all[rows_of(me), cols].astype(F32) + ring1[stage(0, d)].astype(F32)
        for j in range(3):
            total = total + back[j, :, cols].astype(F32)
        out[:, cols] = total.astype(BF16)
        return c

    lax.fori_loop(0, n_db, finish, 0)

    def drain(d, c):
        for j in range(3):
            ret_copy(j, d).wait_send()
        return c

    lax.fori_loop(0, n_db, drain, 0)


def solution(mesh):
    row_spec = P(('dp', 'ep'))
    expert_spec = P('ep')

    def device_step(tokens, expert_ids, gate_vals, w_gate, w_up, w_down):
        tok_dev, d_model = tokens.shape
        n_exp, _, ffn = w_gate.shape
        top_k = expert_ids.shape[1]
        n_tok = GROUPS * tok_dev
        pairs = n_exp * CAP
        units = (n_exp, d_model // KU, KU, ffn)
        hbm = pl.BlockSpec(memory_space=pltpu.HBM)
        dma = pltpu.SemaphoreType.DMA
        return pl.pallas_call(
            layer_kernel,
            out_shape=pltpu.VMEM((tok_dev, d_model), BF16),
            in_specs=[hbm] * 6,
            out_specs=pl.BlockSpec(memory_space=pltpu.VMEM),
            scratch_shapes=[
                pltpu.VMEM((pairs, 2 * ffn), F32),
                pltpu.VMEM((n_tok, d_model), BF16),
                pltpu.VMEM((pairs, ffn), BF16),
                pltpu.VMEM((RING1 + EXTRA, 2, 2, KU, ffn), BF16),
                pltpu.VMEM((RING2, EPS, ffn, DB), BF16),
                pltpu.VMEM((3, tok_dev, d_model), BF16),
                pltpu.VMEM((pairs, DB), BF16),
                pltpu.VMEM((2, 2, 2 * CAP, KU), BF16),
                pltpu.VMEM((top_k, tok_dev), jnp.int32),
                pltpu.VMEM((top_k, tok_dev), F32),
                pltpu.VMEM((3, top_k, tok_dev), jnp.int32),
                pltpu.VMEM((3, top_k, tok_dev), F32),
                pltpu.VMEM((n_exp, n_tok), jnp.int32),
                pltpu.VMEM((8, n_tok), F32),
                dma(((RING1 + EXTRA) // 2,)),
                dma((RING2,)),
                dma((3,)),
                dma((2, 3)),
                dma((2, 3)),
                dma((3, 2 + (d_model // KU - 2) // 2)),
                dma((3, 2 + (d_model // KU - 2) // 2)),
                dma((3, d_model // DB)),
                dma((3, d_model // DB)),
            ],
            compiler_params=pltpu.CompilerParams(collective_id=0, has_side_effects=True, vmem_limit_bytes=65800000),
        )(tokens, expert_ids.T, gate_vals.T, w_gate.reshape(units), w_up.reshape(units), w_down)

    return jax.shard_map(device_step, mesh=mesh, in_specs=(row_spec, row_spec, row_spec, expert_spec, expert_spec, expert_spec), out_specs=row_spec, check_vma=False)
```

```python
import functools

import jax
import jax.numpy as jnp
from jax import lax
from jax.experimental import pallas as pl
from jax.experimental.pallas import tpu as pltpu
from jax.sharding import PartitionSpec as P

MESH = pl.DeviceIdType.MESH
F32, BF16 = jnp.float32, jnp.bfloat16
GROUPS = 4
CAP = 128
KU = 256
DB = 256
RING1 = 8
EXTRA = 4
PER_BODY = 2
EPS = 4
RING2 = 4
FINAL_COLS = 512


def layer_kernel(tok, ids_hbm, gts_hbm, w_gate, w_up, w_down, out, acc, rows_all, hid, ring1, ring2, back,
                 y_blk, xbuf, ids_in, gts_in, ids_all, gts_all, slots, tbl, w1_sem, w2_sem, loc_sem, idx_send, idx_recv, d_send, d_recv,
                 r_send, r_recv):
    tok_dev, d_model = tok.shape
    n_exp, n_unit, _, ffn = w_gate.shape
    n_tok = GROUPS * tok_dev
    n_kb, n_db, n_grp = 2 + (n_unit - 2) // 2, d_model // DB, n_exp // EPS
    n_one, n_two = n_exp // (2 * PER_BODY), n_exp // PER_BODY
    assert EPS % PER_BODY == 0 and n_exp == GROUPS * EPS and n_one * PER_BODY == RING1 == 2 * EXTRA
    steps2 = n_db * n_grp

    me = lax.axis_index('ep')
    sib = me + 1 - 2 * lax.rem(me, 2)
    over = lax.rem(me + 2, GROUPS)
    diag = lax.rem(sib + 2, GROUPS)
    peers = (over, diag, sib)

    def rows_of(dev):
        return pl.ds(pl.multiple_of(dev * tok_dev, tok_dev), tok_dev)

    def first_unit(k):
        return k if isinstance(k, int) and k < 2 else 2 * k - 2

    def pair_of(slot):
        return lax.div(slot, 2)

    def w1_copies(k, i, slot):
        if isinstance(k, int) and k < 2:
            part = (pl.ds(i * 2, 2), k)
        else:
            part = (i, pl.ds(first_unit(k), 2))
        return (pltpu.make_async_copy(w_gate.at[part], ring1.at[slot, 0], w1_sem.at[pair_of(slot)]),
                pltpu.make_async_copy(w_up.at[part], ring1.at[slot, 1], w1_sem.at[pair_of(slot)]))

    def block_cols(k):
        if isinstance(k, int):
            return pl.ds(first_unit(k) * KU, KU if k < 2 else 2 * KU)
        return pl.ds(pl.multiple_of(first_unit(k) * KU, 2 * KU), 2 * KU)

    def w2_copy(step, slot):
        g, d = lax.rem(step, n_grp), lax.div(step, n_grp)
        cols = pl.ds(pl.multiple_of(d * DB, DB), DB)
        return pltpu.make_async_copy(w_down.at[pl.ds(g * EPS, EPS), :, cols], ring2.at[slot], w2_sem.at[slot])

    mine_copy = pltpu.make_async_copy(tok, rows_all.at[rows_of(me), :], loc_sem.at[0])
    ids_copy = pltpu.make_async_copy(ids_hbm, ids_in, loc_sem.at[1])
    gts_copy = pltpu.make_async_copy(gts_hbm, gts_in, loc_sem.at[2])
    ids_copy.start()
    gts_copy.start()
    mine_copy.start()
    barrier = pltpu.get_barrier_semaphore()
    for dev in peers:
        pl.semaphore_signal(barrier, inc=1, device_id={'ep': dev}, device_id_type=MESH)

    def start0(i, c):
        for copy in w1_copies(0, i, i):
            copy.start()
        return c

    lax.fori_loop(0, RING1, start0, 0)
    pl.semaphore_wait(barrier, len(peers))

    def idx_copy(j, what):
        src, dst = (ids_in, ids_all) if what == 0 else (gts_in, gts_all)
        return pltpu.make_async_remote_copy(src_ref=src, dst_ref=dst.at[j], send_sem=idx_send.at[what, j], recv_sem=idx_recv.at[what, j],
                                            device_id={'ep': peers[j]}, device_id_type=MESH)

    def disp_copy(kind, k):
        cols = block_cols(k)
        rows = rows_all.at[rows_of(over if kind == 2 else me), cols]
        return pltpu.make_async_remote_copy(src_ref=rows, dst_ref=rows, send_sem=d_send.at[kind, k], recv_sem=d_recv.at[kind, k],
                                            device_id={'ep': over if kind == 0 else sib}, device_id_type=MESH)

    def disp_arrival(kind, k):
        cols = block_cols(k)
        dst = rows_all.at[rows_of((over, sib, diag)[kind]), cols]
        return pltpu.make_async_remote_copy(src_ref=dst, dst_ref=dst, send_sem=d_send.at[kind, k], recv_sem=d_recv.at[kind, k],
                                            device_id={'ep': over if kind == 0 else sib}, device_id_type=MESH)

    ids_copy.wait()
    gts_copy.wait()
    for j in range(3):
        for what in range(2):
            idx_copy(j, what).start()
    mine_copy.wait()
    for k in range(n_kb):
        disp_copy(0, k).start()
        disp_copy(1, k).start()

    def start1(i, c):
        for copy in w1_copies(1, i, RING1 + i):
            copy.start()
        return c

    def start2(g, c):
        w2_copy(g, g).start()
        return c

    lax.fori_loop(0, EXTRA, start1, 0)
    lax.fori_loop(0, RING2, start2, 0)

    for j in range(3):
        for what in range(2):
            idx_copy(j, what).wait()

    expert = lax.broadcasted_iota(jnp.int32, (n_exp, tok_dev), 0) + me * n_exp

    def side(ids_ref, gts_ref):
        ids, gts = ids_ref[...], gts_ref[...]
        hit_any = jnp.zeros((n_exp, tok_dev), jnp.int32)
        gate = jnp.zeros((n_exp, tok_dev), F32)
        for j in range(ids.shape[0]):
            hit = ids[j:j + 1, :] == expert
            hit_any = hit_any + jnp.where(hit, 1, 0)
            gate = gate + jnp.where(hit, gts[j:j + 1, :], 0.0)
        return hit_any, gate

    parts = [side(ids_in, gts_in)] + [side(ids_all.at[j], gts_all.at[j]) for j in range(3)]

    def of_device(b, i):
        p = [part[i] for part in parts]
        return jnp.where(me == b, p[0], jnp.where(over == b, p[1], jnp.where(diag == b, p[2], p[3])))

    member = jnp.concatenate([of_device(b, 0) for b in range(GROUPS)], axis=1)
    gate = jnp.concatenate([of_device(b, 1) for b in range(GROUPS)], axis=1)
    lane = lax.broadcasted_iota(jnp.int32, (n_exp, n_tok), 1)
    count = member
    shift = 1
    while shift < n_tok:
        count = count + jnp.where(lane >= shift, pltpu.roll(count, shift, 1), 0)
        shift *= 2
    is_mem = member > 0
    slot = jnp.where(is_mem, count - 1, -1)
    slots[...] = slot
    pos = lax.broadcasted_iota(jnp.int32, (n_exp, n_tok), 0) * CAP + slot
    big = n_exp * CAP
    pos1 = jnp.min(jnp.where(is_mem, pos, big), axis=0, keepdims=True)
    pos2 = jnp.max(jnp.where(is_mem, pos, -1), axis=0, keepdims=True)
    g1 = jnp.sum(jnp.where(is_mem & (pos == pos1), gate, 0.0), axis=0, keepdims=True)
    g2 = jnp.sum(jnp.where(is_mem & (pos == pos2), gate, 0.0), axis=0, keepdims=True)
    sub = lax.broadcasted_iota(jnp.int32, (8, n_tok), 0)
    packed = jnp.where(sub == 0, pos1.astype(F32), jnp.where(sub == 1, pos2.astype(F32), jnp.where(sub == 2, g1, jnp.where(sub == 3, g2, 0.0))))
    tbl[...] = packed

    half = big // 2

    def build_picks(i):
        b, h = (i // 2, i % 2) if isinstance(i, int) else (lax.div(i, 2), lax.rem(i, 2))
        per = tok_dev // CAP
        dev, r = (b // per, b % per * CAP) if isinstance(i, int) else (lax.div(b, per), pl.multiple_of(lax.rem(b, per) * CAP, CAP))
        t = jnp.transpose(tbl[:, pl.ds(b * CAP if isinstance(i, int) else pl.multiple_of(b * CAP, CAP), CAP)])
        at = (lax.broadcasted_iota(jnp.int32, (CAP, half), 1) + h * half).astype(F32)
        for p in range(2):
            ring1[RING1 + dev, h, p, pl.ds(r, CAP), :] = jnp.where(t[:, p:p + 1] == at, 1.0, 0.0).astype(BF16)

    def fan(cols, e, n, par):
        at = lax.broadcasted_iota(jnp.int32, (CAP, n_tok), 0)
        for q in range(n // 2):
            hot = jnp.concatenate([jnp.where(at == slots[pl.ds(e + 2 * q + m, 1), :], 1.0, 0.0).astype(BF16) for m in range(2)], axis=0)
            x = jnp.dot(hot, rows_all[:, cols], preferred_element_type=F32).astype(BF16)
            for u in range(x.shape[1] // KU):
                xbuf[par, q + u] = x[:, u * KU:(u + 1) * KU]

    def down(e, ring, i):
        r = pl.ds(pl.multiple_of(e * CAP, CAP), CAP)
        y_blk[r, :] = jnp.dot(hid[r, :], ring2[ring, i], preferred_element_type=F32).astype(BF16)

    def ffn_in(e, rings, par, two, first, final, cw):
        for m in range(len(rings) * (1 if two else 2)):
            ring, xr = rings[m if two else m // 2], pl.ds((m % 2) * CAP, CAP)
            r = pl.ds(pl.multiple_of((e + m) * CAP, CAP), CAP)
            for c0 in range(0, ffn, cw):
                acts = []
                for p in range(2):
                    cols = pl.ds(c0, cw)
                    if two:
                        act = (jnp.dot(xbuf[par, 0, xr, :], ring1[ring, p, 0, :, cols], preferred_element_type=F32) +
                               jnp.dot(xbuf[par, 1, xr, :], ring1[ring, p, 1, :, cols], preferred_element_type=F32))
                    else:
                        act = jnp.dot(xbuf[par, m // 2, xr, :], ring1[ring, p, m % 2, :, cols], preferred_element_type=F32)
                    acc_cols = pl.ds(p * ffn + c0, cw)
                    if not first:
                        act = acc[r, acc_cols] + act
                    if not final:
                        acc[r, acc_cols] = act
                    acts.append(act)
                if final:
                    hid[r, cols] = (jax.nn.silu(acts[0]) * acts[1]).astype(BF16)

    def take(k):
        disp_arrival(1, k).wait_recv()
        disp_arrival(2, k).wait_recv()

    def hand_on(k):
        disp_arrival(0, k).wait_recv()
        disp_copy(2, k).start()

    def begin(k, i):
        rem = (lambda a, b: a % b) if isinstance(i, int) else lax.rem
        slot = i * PER_BODY if k == 0 else rem(i * PER_BODY + k * RING1, RING1 + EXTRA) if k < 3 else rem(i * PER_BODY, RING1)
        both = ring1.at[pl.ds(slot, PER_BODY)]
        pltpu.make_async_copy(both, both, w1_sem.at[pair_of(slot)]).wait()
        return [slot + m for m in range(PER_BODY)]

    def refill(k, i, slot):
        for copy in w1_copies(k, i, slot):
            copy.start()

    def body(k, i, nxt, before=None):
        static = isinstance(i, int)
        two, final = k >= 2, k == n_kb - 1
        per, n_body = (PER_BODY, n_two) if two else (2 * PER_BODY, n_one)
        par = i % 2 if static else lax.rem(i, 2)
        rings = begin(k, i)
        ffn_in(i * per, rings, par, two, k == 0, final, FINAL_COLS if final else ffn)
        if nxt is not None:
            fan(block_cols(nxt[0]), nxt[1] * (PER_BODY if nxt[0] >= 2 else 2 * PER_BODY), PER_BODY if nxt[0] >= 2 else 2 * PER_BODY, 1 - par)
        if before is not None:
            for m in range(PER_BODY):
                e = before * PER_BODY + m
                down(e, lax.div(e, EPS), lax.rem(e, EPS))
        if k == 3:
            for m in range(2):
                build_picks(2 * i + m)

        def fill(kk, i0):
            for m in range(PER_BODY):
                refill(kk, i0 + m, rings[m])

        here, s0 = n_body * PER_BODY, i * PER_BODY
        when = (lambda c: (lambda f: f() if c else None)) if static else pl.when
        if k == 0:
            when(i < 2)(lambda: fill(1, s0 + EXTRA))
            when(i >= 2)(lambda: fill(2, s0 - EXTRA))
        elif k == 1:
            fill(2, s0 + EXTRA)
        elif k == 2:
            when(i < 2)(lambda: fill(2, s0 + RING1 + EXTRA))
            when(i >= 4)(lambda: fill(3, s0 - RING1))
        elif final:
            when(s0 + RING1 < here)(lambda: fill(k, s0 + RING1))
        elif static:
            fill(k + (s0 + RING1) // here, (s0 + RING1) % here)
        else:
            fill(k + lax.div(s0 + RING1, here), lax.rem(s0 + RING1, here))

    hand_on(0)
    take(0)
    fan(block_cols(0), 0, 2 * PER_BODY, 0)
    for k in range(n_kb):
        n_body, final = n_two if k >= 2 else n_one, k == n_kb - 1
        if final:
            for g in range(RING2):
                w2_copy(g, g).wait()

        def loop(i, c, k=k, n_body=n_body, final=final):
            body(k, i, (k, i + 1), lax.rem(i + n_body - 1, n_body) if final else None)
            if not final:
                pl.when(i == n_body - 3)(functools.partial(hand_on, k + 1))
            return c

        lax.fori_loop(0, n_body - 1, loop, 0)
        if not final:
            take(k + 1)
        body(k, n_body - 1, None if final else (k + 1, 0), n_body - 2 if final else None)

    for m in range(EPS - PER_BODY, EPS):
        down(n_exp - EPS + m, n_grp - 1, m)

    def refill2(g, c):
        w2_copy(n_grp + g, g).start()
        return c

    lax.fori_loop(0, RING2, refill2, 0)

    for k in range(n_kb):
        for kind in range(3):
            disp_copy(kind, k).wait_send()

    def stage(slot, d):
        per = ffn // DB
        return (slot, 0, lax.div(d, per), slice(None), pl.ds(pl.multiple_of(lax.rem(d, per) * DB, DB), DB))

    def ret_copy(j, d):
        cols = pl.ds(pl.multiple_of(d * DB, DB), DB)
        return pltpu.make_async_remote_copy(src_ref=rows_all.at[rows_of(peers[j]), cols], dst_ref=back.at[j, :, cols],
                                            send_sem=r_send.at[j, d], recv_sem=r_recv.at[j, d], device_id={'ep': peers[j]}, device_id_type=MESH)

    def combine(d):
        cols = pl.ds(pl.multiple_of(d * DB, DB), DB)

        def one(j, c):
            dev = lax.rem(me + (sib - me) * lax.rem(lax.div(j + 1, 2), 2) + 2 - 2 * lax.div(j, 2), GROUPS)
            r = rows_of(dev)
            y1, y2 = (sum(jnp.dot(ring1[RING1 + dev, h, p], y_blk[h * half:(h + 1) * half, :], preferred_element_type=F32) for h in range(2)) for p in range(2))
            t = jnp.transpose(tbl[:, r])
            sums = (t[:, 2:3] * y1 + t[:, 3:4] * y2).astype(BF16)

            @pl.when(j < 3)
            def _():
                rows_all[r, cols] = sums
                pltpu.make_async_remote_copy(src_ref=rows_all.at[r, cols], dst_ref=back.at[j, :, cols], send_sem=r_send.at[j, d], recv_sem=r_recv.at[j, d],
                                             device_id={'ep': dev}, device_id_type=MESH).start()

            @pl.when(j == 3)
            def _():
                ring1[stage(0, d)] = sums
            return c

        lax.fori_loop(0, GROUPS, one, 0)

    def block2(d, c):
        def step2(g, c2):
            step = d * n_grp + g
            ring = lax.rem(step, RING2)
            w2_copy(step, ring).wait()
            for i in range(EPS):
                down(g * EPS + i, ring, i)

            @pl.when(step + RING2 < steps2)
            def _():
                w2_copy(step + RING2, ring).start()
            return c2

        @pl.when(d > 0)
        def _():
            lax.fori_loop(0, n_grp, step2, 0)

        combine(d)
        return c

    lax.fori_loop(0, n_db, block2, 0)

    def finish(d, c):
        cols = pl.ds(pl.multiple_of(d * DB, DB), DB)
        for j in range(3):
            ret_copy(j, d).wait_recv()
        total = rows_all[rows_of(me), cols].astype(F32) + ring1[stage(0, d)].astype(F32)
        for j in range(3):
            total = total + back[j, :, cols].astype(F32)
        out[:, cols] = total.astype(BF16)
        return c

    lax.fori_loop(0, n_db, finish, 0)

    def drain(d, c):
        for j in range(3):
            ret_copy(j, d).wait_send()
        return c

    lax.fori_loop(0, n_db, drain, 0)


def solution(mesh):
    row_spec = P(('dp', 'ep'))
    expert_spec = P('ep')

    def device_step(tokens, expert_ids, gate_vals, w_gate, w_up, w_down):
        tok_dev, d_model = tokens.shape
        n_exp, _, ffn = w_gate.shape
        top_k = expert_ids.shape[1]
        n_tok = GROUPS * tok_dev
        pairs = n_exp * CAP
        units = (n_exp, d_model // KU, KU, ffn)
        hbm = pl.BlockSpec(memory_space=pltpu.HBM)
        dma = pltpu.SemaphoreType.DMA
        return pl.pallas_call(
            layer_kernel,
            out_shape=pltpu.VMEM((tok_dev, d_model), BF16),
            in_specs=[hbm] * 6,
            out_specs=pl.BlockSpec(memory_space=pltpu.VMEM),
            scratch_shapes=[
                pltpu.VMEM((pairs, 2 * ffn), F32),
                pltpu.VMEM((n_tok, d_model), BF16),
                pltpu.VMEM((pairs, ffn), BF16),
                pltpu.VMEM((RING1 + EXTRA, 2, 2, KU, ffn), BF16),
                pltpu.VMEM((RING2, EPS, ffn, DB), BF16),
                pltpu.VMEM((3, tok_dev, d_model), BF16),
                pltpu.VMEM((pairs, DB), BF16),
                pltpu.VMEM((2, 2, 2 * CAP, KU), BF16),
                pltpu.VMEM((top_k, tok_dev), jnp.int32),
                pltpu.VMEM((top_k, tok_dev), F32),
                pltpu.VMEM((3, top_k, tok_dev), jnp.int32),
                pltpu.VMEM((3, top_k, tok_dev), F32),
                pltpu.VMEM((n_exp, n_tok), jnp.int32),
                pltpu.VMEM((8, n_tok), F32),
                dma(((RING1 + EXTRA) // 2,)),
                dma((RING2,)),
                dma((3,)),
                dma((2, 3)),
                dma((2, 3)),
                dma((3, 2 + (d_model // KU - 2) // 2)),
                dma((3, 2 + (d_model // KU - 2) // 2)),
                dma((3, d_model // DB)),
                dma((3, d_model // DB)),
            ],
            compiler_params=pltpu.CompilerParams(collective_id=0, has_side_effects=True, vmem_limit_bytes=65800000),
        )(tokens, expert_ids.T, gate_vals.T, w_gate.reshape(units), w_up.reshape(units), w_down)

    return jax.shard_map(device_step, mesh=mesh, in_specs=(row_spec, row_spec, row_spec, expert_spec, expert_spec, expert_spec), out_specs=row_spec, check_vma=False)
```

```python
import functools

import jax
import jax.numpy as jnp
from jax import lax
from jax.experimental import pallas as pl
from jax.experimental.pallas import tpu as pltpu
from jax.sharding import PartitionSpec as P

MESH = pl.DeviceIdType.MESH
F32, BF16 = jnp.float32, jnp.bfloat16
GROUPS = 4
CAP = 128
KU = 256
DB = 256
RING1 = 8
EXTRA = 4
PER_BODY = 2
EPS = 4
RING2 = 4
FINAL_COLS = 512


def layer_kernel(tok, ids_hbm, gts_hbm, w_gate, w_up, w_down, out, acc, rows_all, hid, ring1, ring2, back,
                 y_blk, xbuf, ids_in, gts_in, ids_all, gts_all, slots, tbl, w1_sem, w2_sem, loc_sem, idx_send, idx_recv, d_send, d_recv,
                 r_send, r_recv):
    tok_dev, d_model = tok.shape
    n_exp, n_unit, _, ffn = w_gate.shape
    n_tok = GROUPS * tok_dev
    n_kb, n_db, n_grp = 2 + (n_unit - 2) // 2, d_model // DB, n_exp // EPS
    n_one, n_two = n_exp // (2 * PER_BODY), n_exp // PER_BODY
    assert EPS % PER_BODY == 0 and n_exp == GROUPS * EPS and n_one * PER_BODY == RING1 == 2 * EXTRA
    steps2 = n_db * n_grp

    me = lax.axis_index('ep')
    sib = me + 1 - 2 * lax.rem(me, 2)
    over = lax.rem(me + 2, GROUPS)
    diag = lax.rem(sib + 2, GROUPS)
    peers = (over, diag, sib)

    def rows_of(dev):
        return pl.ds(pl.multiple_of(dev * tok_dev, tok_dev), tok_dev)

    def first_unit(k):
        return k if isinstance(k, int) and k < 2 else 2 * k - 2

    def pair_of(slot):
        return lax.div(slot, 2)

    def w1_copies(k, i, slot):
        if isinstance(k, int) and k < 2:
            part = (pl.ds(i * 2, 2), k)
        else:
            part = (i, pl.ds(first_unit(k), 2))
        return (pltpu.make_async_copy(w_gate.at[part], ring1.at[slot, 0], w1_sem.at[pair_of(slot)]),
                pltpu.make_async_copy(w_up.at[part], ring1.at[slot, 1], w1_sem.at[pair_of(slot)]))

    def block_cols(k):
        if isinstance(k, int):
            return pl.ds(first_unit(k) * KU, KU if k < 2 else 2 * KU)
        return pl.ds(pl.multiple_of(first_unit(k) * KU, 2 * KU), 2 * KU)

    def w2_copy(step, slot):
        g, d = lax.rem(step, n_grp), lax.div(step, n_grp)
        cols = pl.ds(pl.multiple_of(d * DB, DB), DB)
        return pltpu.make_async_copy(w_down.at[pl.ds(g * EPS, EPS), :, cols], ring2.at[slot], w2_sem.at[slot])

    mine_copy = pltpu.make_async_copy(tok, rows_all.at[rows_of(me), :], loc_sem.at[0])
    ids_copy = pltpu.make_async_copy(ids_hbm, ids_in, loc_sem.at[1])
    gts_copy = pltpu.make_async_copy(gts_hbm, gts_in, loc_sem.at[2])
    ids_copy.start()
    gts_copy.start()
    mine_copy.start()
    barrier = pltpu.get_barrier_semaphore()
    for dev in peers:
        pl.semaphore_signal(barrier, inc=1, device_id={'ep': dev}, device_id_type=MESH)

    def start0(i, c):
        for copy in w1_copies(0, i, i):
            copy.start()
        return c

    lax.fori_loop(0, RING1, start0, 0)
    pl.semaphore_wait(barrier, len(peers))

    def idx_copy(j, what):
        src, dst = (ids_in, ids_all) if what == 0 else (gts_in, gts_all)
        return pltpu.make_async_remote_copy(src_ref=src, dst_ref=dst.at[j], send_sem=idx_send.at[what, j], recv_sem=idx_recv.at[what, j],
                                            device_id={'ep': peers[j]}, device_id_type=MESH)

    def disp_copy(kind, k):
        cols = block_cols(k)
        rows = rows_all.at[rows_of(over if kind == 2 else me), cols]
        return pltpu.make_async_remote_copy(src_ref=rows, dst_ref=rows, send_sem=d_send.at[kind, k], recv_sem=d_recv.at[kind, k],
                                            device_id={'ep': over if kind == 0 else sib}, device_id_type=MESH)

    def disp_arrival(kind, k):
        cols = block_cols(k)
        dst = rows_all.at[rows_of((over, sib, diag)[kind]), cols]
        return pltpu.make_async_remote_copy(src_ref=dst, dst_ref=dst, send_sem=d_send.at[kind, k], recv_sem=d_recv.at[kind, k],
                                            device_id={'ep': over if kind == 0 else sib}, device_id_type=MESH)

    ids_copy.wait()
    gts_copy.wait()
    for j in range(3):
        for what in range(2):
            idx_copy(j, what).start()
    mine_copy.wait()
    for k in range(n_kb):
        disp_copy(0, k).start()
        disp_copy(1, k).start()

    def start1(i, c):
        for copy in w1_copies(1, i, RING1 + i):
            copy.start()
        return c

    def start2(g, c):
        w2_copy(g, g).start()
        return c

    lax.fori_loop(0, EXTRA, start1, 0)
    lax.fori_loop(0, RING2, start2, 0)

    for j in range(3):
        for what in range(2):
            idx_copy(j, what).wait()

    expert = lax.broadcasted_iota(jnp.int32, (n_exp, tok_dev), 0) + me * n_exp

    def side(ids_ref, gts_ref):
        ids, gts = ids_ref[...], gts_ref[...]
        hit_any = jnp.zeros((n_exp, tok_dev), jnp.int32)
        gate = jnp.zeros((n_exp, tok_dev), F32)
        for j in range(ids.shape[0]):
            hit = ids[j:j + 1, :] == expert
            hit_any = hit_any + jnp.where(hit, 1, 0)
            gate = gate + jnp.where(hit, gts[j:j + 1, :], 0.0)
        return hit_any, gate

    parts = [side(ids_in, gts_in)] + [side(ids_all.at[j], gts_all.at[j]) for j in range(3)]

    def of_device(b, i):
        p = [part[i] for part in parts]
        return jnp.where(me == b, p[0], jnp.where(over == b, p[1], jnp.where(diag == b, p[2], p[3])))

    member = jnp.concatenate([of_device(b, 0) for b in range(GROUPS)], axis=1)
    gate = jnp.concatenate([of_device(b, 1) for b in range(GROUPS)], axis=1)
    lane = lax.broadcasted_iota(jnp.int32, (n_exp, n_tok), 1)
    count = member
    shift = 1
    while shift < n_tok:
        count = count + jnp.where(lane >= shift, pltpu.roll(count, shift, 1), 0)
        shift *= 2
    is_mem = member > 0
    slot = jnp.where(is_mem, count - 1, -1)
    slots[...] = slot
    pos = lax.broadcasted_iota(jnp.int32, (n_exp, n_tok), 0) * CAP + slot
    big = n_exp * CAP
    pos1 = jnp.min(jnp.where(is_mem, pos, big), axis=0, keepdims=True)
    pos2 = jnp.max(jnp.where(is_mem, pos, -1), axis=0, keepdims=True)
    g1 = jnp.sum(jnp.where(is_mem & (pos == pos1), gate, 0.0), axis=0, keepdims=True)
    g2 = jnp.sum(jnp.where(is_mem & (pos == pos2), gate, 0.0), axis=0, keepdims=True)
    sub = lax.broadcasted_iota(jnp.int32, (8, n_tok), 0)
    packed = jnp.where(sub == 0, pos1.astype(F32), jnp.where(sub == 1, pos2.astype(F32), jnp.where(sub == 2, g1, jnp.where(sub == 3, g2, 0.0))))
    tbl[...] = packed

    half = big // 2

    def build_picks(i):
        b, h = (i // 2, i % 2) if isinstance(i, int) else (lax.div(i, 2), lax.rem(i, 2))
        per = tok_dev // CAP
        dev, r = (b // per, b % per * CAP) if isinstance(i, int) else (lax.div(b, per), pl.multiple_of(lax.rem(b, per) * CAP, CAP))
        t = jnp.transpose(tbl[:, pl.ds(b * CAP if isinstance(i, int) else pl.multiple_of(b * CAP, CAP), CAP)])
        at = (lax.broadcasted_iota(jnp.int32, (CAP, half), 1) + h * half).astype(F32)
        for p in range(2):
            ring1[RING1 + dev, h, p, pl.ds(r, CAP), :] = jnp.where(t[:, p:p + 1] == at, 1.0, 0.0).astype(BF16)

    near, far = (pl.ds(pl.multiple_of(c * 2 * tok_dev, 2 * tok_dev), 2 * tok_dev) for c in (lax.div(me, 2), 1 - lax.div(me, 2)))

    def gather(cols, e, tokens):
        at = lax.broadcasted_iota(jnp.int32, (CAP, n_tok if tokens is None else 2 * tok_dev), 0)
        tokens = slice(None) if tokens is None else tokens
        hot = jnp.concatenate([jnp.where(at == slots[pl.ds(e + m, 1), tokens], 1.0, 0.0).astype(BF16) for m in range(2)], axis=0)
        return jnp.dot(hot, rows_all[tokens, cols], preferred_element_type=F32)

    def gather_near(col0, width):
        def pair(i, c):
            hid[pl.ds(pl.multiple_of(i * 2 * CAP, 2 * CAP), 2 * CAP), pl.ds(col0, width)] = gather(pl.ds(col0, width), i * 2, near).astype(BF16)
            return c

        lax.fori_loop(0, n_exp // 2, pair, 0)

    def fan(k, e, n, par):
        cols = block_cols(k)
        for q in range(n // 2):
            if k < 3:
                rows = pl.ds((e + 2 * q) * CAP if isinstance(e, int) else pl.multiple_of((e + 2 * q) * CAP, 2 * CAP), 2 * CAP)
                x = (gather(cols, e + 2 * q, far) + hid[rows, cols].astype(F32)).astype(BF16)
            else:
                x = gather(cols, e + 2 * q, None).astype(BF16)
            for u in range(x.shape[1] // KU):
                xbuf[par, q + u] = x[:, u * KU:(u + 1) * KU]

    def down(e, ring, i):
        r = pl.ds(pl.multiple_of(e * CAP, CAP), CAP)
        y_blk[r, :] = jnp.dot(hid[r, :], ring2[ring, i], preferred_element_type=F32).astype(BF16)

    def ffn_in(e, rings, par, two, first, final, cw):
        for m in range(len(rings) * (1 if two else 2)):
            ring, xr = rings[m if two else m // 2], pl.ds((m % 2) * CAP, CAP)
            r = pl.ds(pl.multiple_of((e + m) * CAP, CAP), CAP)
            for c0 in range(0, ffn, cw):
                acts = []
                for p in range(2):
                    cols = pl.ds(c0, cw)
                    if two:
                        act = (jnp.dot(xbuf[par, 0, xr, :], ring1[ring, p, 0, :, cols], preferred_element_type=F32) +
                               jnp.dot(xbuf[par, 1, xr, :], ring1[ring, p, 1, :, cols], preferred_element_type=F32))
                    else:
                        act = jnp.dot(xbuf[par, m // 2, xr, :], ring1[ring, p, m % 2, :, cols], preferred_element_type=F32)
                    acc_cols = pl.ds(p * ffn + c0, cw)
                    if not first:
                        act = acc[r, acc_cols] + act
                    if not final:
                        acc[r, acc_cols] = act
                    acts.append(act)
                if final:
                    hid[r, cols] = (jax.nn.silu(acts[0]) * acts[1]).astype(BF16)

    def take(k):
        if k >= 3:
            disp_arrival(1, k).wait_recv()
        disp_arrival(2, k).wait_recv()

    def hand_on(k):
        disp_arrival(0, k).wait_recv()
        disp_copy(2, k).start()

    def begin(k, i):
        rem = (lambda a, b: a % b) if isinstance(i, int) else lax.rem
        slot = i * PER_BODY if k == 0 else rem(i * PER_BODY + k * RING1, RING1 + EXTRA) if k < 3 else rem(i * PER_BODY, RING1)
        both = ring1.at[pl.ds(slot, PER_BODY)]
        pltpu.make_async_copy(both, both, w1_sem.at[pair_of(slot)]).wait()
        return [slot + m for m in range(PER_BODY)]

    def refill(k, i, slot):
        for copy in w1_copies(k, i, slot):
            copy.start()

    def body(k, i, nxt, before=None):
        static = isinstance(i, int)
        two, final = k >= 2, k == n_kb - 1
        per, n_body = (PER_BODY, n_two) if two else (2 * PER_BODY, n_one)
        par = i % 2 if static else lax.rem(i, 2)
        rings = begin(k, i)
        ffn_in(i * per, rings, par, two, k == 0, final, 512)
        if nxt is not None:
            fan(nxt[0], nxt[1] * (PER_BODY if nxt[0] >= 2 else 2 * PER_BODY), PER_BODY if nxt[0] >= 2 else 2 * PER_BODY, 1 - par)
        if before is not None:
            for m in range(PER_BODY):
                e = before * PER_BODY + m
                down(e, lax.div(e, EPS), lax.rem(e, EPS))
        if k == 3:
            for m in range(2):
                build_picks(2 * i + m)

        def fill(kk, i0):
            for m in range(PER_BODY):
                refill(kk, i0 + m, rings[m])

        here, s0 = n_body * PER_BODY, i * PER_BODY
        when = (lambda c: (lambda f: f() if c else None)) if static else pl.when
        if k == 0:
            when(i < 2)(lambda: fill(1, s0 + EXTRA))
            when(i >= 2)(lambda: fill(2, s0 - EXTRA))
        elif k == 1:
            fill(2, s0 + EXTRA)
        elif k == 2:
            when(i < 2)(lambda: fill(2, s0 + RING1 + EXTRA))
            when(i >= 4)(lambda: fill(3, s0 - RING1))
        elif final:
            when(s0 + RING1 < here)(lambda: fill(k, s0 + RING1))
        elif static:
            fill(k + (s0 + RING1) // here, (s0 + RING1) % here)
        else:
            fill(k + lax.div(s0 + RING1, here), lax.rem(s0 + RING1, here))

    for k in range(3):
        disp_arrival(1, k).wait_recv()
    gather_near(0, 2 * KU)
    hand_on(0)
    gather_near(2 * KU, 2 * KU)
    take(0)
    fan(0, 0, 2 * PER_BODY, 0)
    for k in range(n_kb):
        n_body, final = n_two if k >= 2 else n_one, k == n_kb - 1
        if final:
            for g in range(RING2):
                w2_copy(g, g).wait()

        def loop(i, c, k=k, n_body=n_body, final=final):
            body(k, i, (k, i + 1), lax.rem(i + n_body - 1, n_body) if final else None)
            if not final:
                pl.when(i == n_body - 3)(functools.partial(hand_on, k + 1))
            return c

        lax.fori_loop(0, n_body - 1, loop, 0)
        if not final:
            take(k + 1)
        body(k, n_body - 1, None if final else (k + 1, 0), n_body - 2 if final else None)

    for m in range(EPS - PER_BODY, EPS):
        down(n_exp - EPS + m, n_grp - 1, m)

    def refill2(g, c):
        w2_copy(n_grp + g, g).start()
        return c

    lax.fori_loop(0, RING2, refill2, 0)

    for k in range(n_kb):
        for kind in range(3):
            disp_copy(kind, k).wait_send()

    def stage(slot, d):
        per = ffn // DB
        return (slot, 0, lax.div(d, per), slice(None), pl.ds(pl.multiple_of(lax.rem(d, per) * DB, DB), DB))

    def ret_copy(j, d):
        cols = pl.ds(pl.multiple_of(d * DB, DB), DB)
        return pltpu.make_async_remote_copy(src_ref=rows_all.at[rows_of(peers[j]), cols], dst_ref=back.at[j, :, cols],
                                            send_sem=r_send.at[j, d], recv_sem=r_recv.at[j, d], device_id={'ep': peers[j]}, device_id_type=MESH)

    def combine(d):
        cols = pl.ds(pl.multiple_of(d * DB, DB), DB)

        def one(j, c):
            dev = lax.rem(me + (sib - me) * lax.rem(lax.div(j + 1, 2), 2) + 2 - 2 * lax.div(j, 2), GROUPS)
            r = rows_of(dev)
            y1, y2 = (sum(jnp.dot(ring1[RING1 + dev, h, p], y_blk[h * half:(h + 1) * half, :], preferred_element_type=F32) for h in range(2)) for p in range(2))
            t = jnp.transpose(tbl[:, r])
            sums = (t[:, 2:3] * y1 + t[:, 3:4] * y2).astype(BF16)

            @pl.when(j < 3)
            def _():
                rows_all[r, cols] = sums
                pltpu.make_async_remote_copy(src_ref=rows_all.at[r, cols], dst_ref=back.at[j, :, cols], send_sem=r_send.at[j, d], recv_sem=r_recv.at[j, d],
                                             device_id={'ep': dev}, device_id_type=MESH).start()

            @pl.when(j == 3)
            def _():
                ring1[stage(0, d)] = sums
            return c

        lax.fori_loop(0, GROUPS, one, 0)

    def block2(d, c):
        def step2(g, c2):
            step = d * n_grp + g
            ring = lax.rem(step, RING2)
            w2_copy(step, ring).wait()
            for i in range(EPS):
                down(g * EPS + i, ring, i)

            @pl.when(step + RING2 < steps2)
            def _():
                w2_copy(step + RING2, ring).start()
            return c2

        @pl.when(d > 0)
        def _():
            lax.fori_loop(0, n_grp, step2, 0)

        combine(d)
        return c

    lax.fori_loop(0, n_db, block2, 0)

    def finish(d, c):
        cols = pl.ds(pl.multiple_of(d * DB, DB), DB)
        for j in range(3):
            ret_copy(j, d).wait_recv()
        total = rows_all[rows_of(me), cols].astype(F32) + ring1[stage(0, d)].astype(F32)
        for j in range(3):
            total = total + back[j, :, cols].astype(F32)
        out[:, cols] = total.astype(BF16)
        return c

    lax.fori_loop(0, n_db, finish, 0)

    def drain(d, c):
        for j in range(3):
            ret_copy(j, d).wait_send()
        return c

    lax.fori_loop(0, n_db, drain, 0)


def solution(mesh):
    row_spec = P(('dp', 'ep'))
    expert_spec = P('ep')

    def device_step(tokens, expert_ids, gate_vals, w_gate, w_up, w_down):
        tok_dev, d_model = tokens.shape
        n_exp, _, ffn = w_gate.shape
        top_k = expert_ids.shape[1]
        n_tok = GROUPS * tok_dev
        pairs = n_exp * CAP
        units = (n_exp, d_model // KU, KU, ffn)
        hbm = pl.BlockSpec(memory_space=pltpu.HBM)
        dma = pltpu.SemaphoreType.DMA
        return pl.pallas_call(
            layer_kernel,
            out_shape=pltpu.VMEM((tok_dev, d_model), BF16),
            in_specs=[hbm] * 6,
            out_specs=pl.BlockSpec(memory_space=pltpu.VMEM),
            scratch_shapes=[
                pltpu.VMEM((pairs, 2 * ffn), F32),
                pltpu.VMEM((n_tok, d_model), BF16),
                pltpu.VMEM((pairs, ffn), BF16),
                pltpu.VMEM((RING1 + EXTRA, 2, 2, KU, ffn), BF16),
                pltpu.VMEM((RING2, EPS, ffn, DB), BF16),
                pltpu.VMEM((3, tok_dev, d_model), BF16),
                pltpu.VMEM((pairs, DB), BF16),
                pltpu.VMEM((2, 2, 2 * CAP, KU), BF16),
                pltpu.VMEM((top_k, tok_dev), jnp.int32),
                pltpu.VMEM((top_k, tok_dev), F32),
                pltpu.VMEM((3, top_k, tok_dev), jnp.int32),
                pltpu.VMEM((3, top_k, tok_dev), F32),
                pltpu.VMEM((n_exp, n_tok), jnp.int32),
                pltpu.VMEM((8, n_tok), F32),
                dma(((RING1 + EXTRA) // 2,)),
                dma((RING2,)),
                dma((3,)),
                dma((2, 3)),
                dma((2, 3)),
                dma((3, 2 + (d_model // KU - 2) // 2)),
                dma((3, 2 + (d_model // KU - 2) // 2)),
                dma((3, d_model // DB)),
                dma((3, d_model // DB)),
            ],
            compiler_params=pltpu.CompilerParams(collective_id=0, has_side_effects=True, vmem_limit_bytes=65800000),
        )(tokens, expert_ids.T, gate_vals.T, w_gate.reshape(units), w_up.reshape(units), w_down)

    return jax.shard_map(device_step, mesh=mesh, in_specs=(row_spec, row_spec, row_spec, expert_spec, expert_spec, expert_spec), out_specs=row_spec, check_vma=False)
```
